256 devices in a mesh: pair: 64 (over z, x, core), mp: 4 (over y).
Axes of the slice: x: 4, y: 4, z: 8, core: 2. Of those that a mesh axis runs over, the one named last changes fastest.
Arguments:
- current: bfloat16 [128, 196, 1024], P('pair'), may hold values from -6 to 6
- past_tokens: bfloat16 [128, 196, 1024], P('pair'), may hold values from -6 to 6
- counts: int32 [128], P('pair'), may hold values from 1 to 196, as said below
- partners: int32 [128], replicated, may hold values from 0 to 127, as said below
- query_weight: bfloat16 [1024, 1024], P(None, 'mp'), may hold values from -1.2 to 1.2
- key_weight: bfloat16 [1024, 1024], P(None, 'mp'), may hold values from -1.2 to 1.2
- value_weight: bfloat16 [1024, 1024], P(None, 'mp'), may hold values from -0.1875 to 0.1875
- output_weight: bfloat16 [1024, 1024], P('mp'), may hold values from -0.1875 to 0.1875
- up_weight: bfloat16 [1024, 4096], P(None, 'mp'), may hold values from -0.1875 to 0.1875
- down_weight: bfloat16 [4096, 1024], P('mp'), may hold values from -0.09375 to 0.09375
Outputs:
- decoded: bfloat16 [128, 196, 1024], P('pair', None, 'mp')
The draws below stay inside these ranges and needn't reach their ends.
Inputs may be any that keep to these rules, and one draw needn't show every extreme that they name: counts[p] is at most 196; some pair has exactly 196. A permutation of the pairs; partners[p] % 2 == p % 2; the partners of the 2 pairs of one pair index lie on distinct pair indices, and the pairs whose partners lie on one pair index come from distinct pair indices.
All inputs are finite; a program needn't handle non-finite values.
Results may differ from the reference program's by a relative error of at most 0.0085.
Values may be sent and summed in bfloat16 or wider, within the bound.
A program may use at most 128 MiB of HBM per device.

```python
import jax
import jax.numpy as jnp
from jax import lax

D = 1024
HEADS = 16
HEAD_DIM = 64
FF = 4096
KEYS = 196
QSLOT = 196
PAIR_DEV = 2
PAIRS = 128


def pairing(key):
    groups = PAIRS // PAIR_DEV
    leading = jax.random.permutation(jax.random.fold_in(key, 11), groups)
    stride = 1 + jax.random.randint(jax.random.fold_in(key, 12), (), 0, max(groups // PAIR_DEV - 1, 1))
    positions = jnp.arange(PAIRS, dtype=jnp.int32)
    slot_of = positions % PAIR_DEV
    owner_of = positions // PAIR_DEV
    partner = (leading[owner_of] + slot_of * stride) % groups
    return (partner * PAIR_DEV + slot_of).astype(jnp.int32)


def past_rows(key):
    values = jnp.clip(jax.random.normal(jax.random.fold_in(key, 13), (PAIRS, KEYS, D), jnp.float32), -6.0, 6.0)
    return values


def query_key(key):
    common = jax.random.normal(jax.random.fold_in(key, 31), (D, D), jnp.float32)
    private = jax.random.normal(jax.random.fold_in(key, 32), (D, D), jnp.float32)
    query_part = common * D ** (-0.5)
    key_part = private * D ** (-0.5)
    return (jnp.clip(query_part, -1.2, 1.2), jnp.clip(key_part, -1.2, 1.2))


def draw_partners(key, part):
    return pairing(key)


def draw_past_tokens(key, part):
    return past_rows(key).astype(jnp.bfloat16)


def draw_current(key, part):
    values = jnp.clip(jax.random.normal(jax.random.fold_in(key, 21), (PAIRS, QSLOT, D), jnp.float32), -6.0, 6.0)
    return values.astype(jnp.bfloat16)


def draw_counts(key, part):
    drawn = jax.random.randint(jax.random.fold_in(key, 41), (PAIRS,), 0, KEYS)
    counts = KEYS - drawn * drawn // KEYS
    chosen = jax.random.randint(jax.random.fold_in(key, 42), (), 0, PAIRS)
    return jnp.where(jnp.arange(PAIRS, dtype=jnp.int32) == chosen, KEYS, counts).astype(jnp.int32)


def draw_query_weight(key, part):
    return query_key(key)[0].astype(jnp.bfloat16)


def draw_key_weight(key, part):
    return query_key(key)[1].astype(jnp.bfloat16)


def level_of(key, dims, cuts, least, top_value):
    loudness, own = 1.0, jax.random.fold_in(key, 6)
    for axis_at, parts in cuts:
        steps = jnp.exp(jax.random.uniform(jax.random.fold_in(own, axis_at), (parts,), jnp.float32, least / len(cuts), top_value / len(cuts)))
        loudness = loudness * jnp.repeat(steps, dims[axis_at] // parts).reshape([-1 if axis == axis_at else 1 for axis in range(len(dims))])
    return loudness


def bell_draw(rng, shape, width, limit, shards=(), held_as=jnp.bfloat16):
    values = width * jax.random.normal(rng, shape, jnp.float32)
    if shards:
        values = values * level_of(rng, shape, shards, -0.22, 0.18)
    return jnp.clip(values, -limit, limit).astype(held_as)


def setup_inputs(seed: int = 0) -> dict:
    key_of = jax.random.split(jax.random.key(seed), 11)
    current = draw_current(jax.random.fold_in(key_of[10], 71), 0)
    past_tokens = draw_past_tokens(jax.random.fold_in(key_of[10], 71), 0)
    counts = draw_counts(jax.random.fold_in(key_of[10], 71), 0)
    partners = draw_partners(jax.random.fold_in(key_of[10], 71), 0)
    query_weight = draw_query_weight(jax.random.fold_in(key_of[10], 71), 0)
    key_weight = draw_key_weight(jax.random.fold_in(key_of[10], 71), 0)
    value_weight = bell_draw(key_of[6], (D, D), D ** -0.5, 0.1875, ((1, 4),))
    output_weight = bell_draw(key_of[7], (D, D), D ** -0.5, 0.1875, ((0, 4),))
    up_weight = bell_draw(key_of[8], (D, FF), D ** -0.5, 0.1875, ((1, 4),))
    down_weight = bell_draw(key_of[9], (FF, D), FF ** -0.5, 0.09375, ((0, 4),))
    return dict(current=current, past_tokens=past_tokens, counts=counts, partners=partners, query_weight=query_weight, key_weight=key_weight, value_weight=value_weight, output_weight=output_weight, up_weight=up_weight, down_weight=down_weight)


def layer_norm(values):
    center = values - lax.optimization_barrier(jnp.mean(values, axis=-1, keepdims=True))
    spread = lax.optimization_barrier(jnp.mean(center * center, axis=-1, keepdims=True))
    return center * lax.rsqrt(spread + 1e-06)

def attend(inputs):
    query_block, key_block, value_block = inputs
    scores = jnp.einsum('qhd,khd->hqk', query_block.astype(jnp.float32), key_block.astype(jnp.float32)) * HEAD_DIM ** (-0.5)
    row_max = lax.optimization_barrier(jnp.max(scores, axis=-1, keepdims=True))
    lifted = jnp.exp(scores - row_max)
    weights = (lifted / lax.optimization_barrier(jnp.sum(lifted, axis=-1, keepdims=True))).astype(jnp.bfloat16)
    return jnp.einsum('hqk,khd->qhd', weights.astype(jnp.float32), value_block.astype(jnp.float32)).astype(jnp.bfloat16)

def reference(current, past_tokens, counts, partners, query_weight, key_weight, value_weight, output_weight, up_weight, down_weight):
    model_width = current.shape[2]
    normed = layer_norm(current.astype(jnp.float32)).astype(jnp.bfloat16).reshape(-1, model_width)
    context = layer_norm(past_tokens.astype(jnp.float32)).astype(jnp.bfloat16).reshape(-1, model_width)
    queries = jnp.dot(normed, query_weight, preferred_element_type=jnp.float32).astype(jnp.bfloat16).reshape(PAIRS, QSLOT, HEADS, HEAD_DIM)
    keys_all = jnp.dot(context, key_weight, preferred_element_type=jnp.float32).astype(jnp.bfloat16).reshape(PAIRS, KEYS, HEADS, HEAD_DIM)
    values_all = jnp.dot(context, value_weight, preferred_element_type=jnp.float32).astype(jnp.bfloat16).reshape(PAIRS, KEYS, HEADS, HEAD_DIM)
    attended = lax.map(attend, (queries, keys_all[partners], values_all[partners]))
    projected = jnp.dot(attended.reshape(-1, model_width), output_weight, preferred_element_type=jnp.float32)
    hidden = current.astype(jnp.float32).reshape(-1, model_width) + projected
    mixer_in = layer_norm(hidden).astype(jnp.bfloat16)
    expanded = jax.nn.gelu(jnp.dot(mixer_in, up_weight, preferred_element_type=jnp.float32), approximate=False).astype(jnp.bfloat16)
    result = hidden + jnp.dot(expanded, down_weight, preferred_element_type=jnp.float32)
    is_live = (jnp.arange(QSLOT, dtype=jnp.int32)[None, :] < counts[:, None]).reshape(-1, 1)
    result = jnp.where(is_live, result, 0.0)
    return result.reshape(PAIRS, QSLOT, model_width).astype(jnp.bfloat16)
```

```python
import functools

import jax
import jax.numpy as jnp
from jax import lax
from jax.experimental import pallas as pl
from jax.experimental.pallas import tpu as pltpu
from jax.sharding import PartitionSpec as P

HEAD_DIM = 64
TILE = 16
LANES = 128
MESH = pl.DeviceIdType.MESH


def exchange_kernel(
    groups,
    shards,
    partners_ref,
    past_ref,
    out_ref,
    spread,
    sorted_tiles,
    context,
    send_one,
    recv_one,
    send_two,
    recv_two,
    ring_send,
    ring_recv,
):
    slots, rows, width = past_ref.shape
    share = width // shards
    halves = share // LANES
    blocks = rows // TILE
    kinds = slots * blocks * halves
    me = lax.axis_index("pair")
    rank = lax.axis_index("mp")
    column = rank * share
    after = lax.rem(rank + 1, shards)
    before = lax.rem(rank + shards - 1, shards)

    def keeper(kind):
        return (kind * groups) // kinds

    mine = (me * kinds + groups - 1) // groups
    keeps = jnp.logical_and(mine < kinds, keeper(mine) == me)

    def place(kind):
        slot = kind // (blocks * halves)
        left = kind % (blocks * halves)
        row = pl.multiple_of((left // halves) * TILE, TILE)
        lane = pl.multiple_of(column + (left % halves) * LANES, LANES)
        return slot, pl.ds(row, TILE), pl.ds(lane, LANES)

    barrier = pltpu.get_barrier_semaphore()

    def greet(step, carry):
        peer = lax.rem(me + 1 + step, groups)
        pl.semaphore_signal(barrier, inc=1, device_id={"pair": peer}, device_id_type=MESH)
        return carry

    lax.fori_loop(0, groups - 1, greet, 0)
    for peer in (after, before):
        pl.semaphore_signal(barrier, inc=1, device_id={"mp": peer}, device_id_type=MESH)
    pl.semaphore_wait(barrier, groups + 1)

    first = (me * kinds) // groups

    def spread_one(step, carry):
        kind = lax.rem(first + step, kinds)
        target = keeper(kind)
        slot, row, lane = place(kind)

        @pl.when(target != me)
        def _():
            pltpu.make_async_remote_copy(
                src_ref=past_ref.at[slot, row, lane],
                dst_ref=spread.at[me],
                send_sem=send_one,
                recv_sem=recv_one,
                device_id={"pair": target},
                device_id_type=MESH,
            ).start()

        @pl.when(target == me)
        def _():
            spread[me] = past_ref[slot, row, lane]

        return carry

    lax.fori_loop(0, kinds, spread_one, 0)

    @pl.when(keeps)
    def _():
        slot, row, lane = place(mine)
        arrived = spread.at[pl.ds(0, groups - 1)]
        pltpu.make_async_copy(arrived, arrived, recv_one).wait()

        def sort_one(step, carry):
            owner = partners_ref[step * slots + slot] // slots
            sorted_tiles[step] = spread[owner]
            return carry

        lax.fori_loop(0, groups, sort_one, 0)
        context[slot, row, lane] = sorted_tiles[me]

        def deliver(step, carry):
            target = lax.rem(me + 1 + step, groups)
            pltpu.make_async_remote_copy(
                src_ref=sorted_tiles.at[target],
                dst_ref=context.at[slot, row, lane],
                send_sem=send_two,
                recv_sem=recv_two,
                device_id={"pair": target},
                device_id_type=MESH,
            ).start()
            return carry

        lax.fori_loop(0, groups - 1, deliver, 0)
        left = spread.at[pl.ds(0, kinds - 1)]
        pltpu.make_async_copy(left, left, send_one).wait()
        got = spread.at[pl.ds(0, kinds - 1)]
        pltpu.make_async_copy(got, got, recv_two).wait()
        sent = spread.at[pl.ds(0, groups - 1)]
        pltpu.make_async_copy(sent, sent, send_two).wait()

    @pl.when(jnp.logical_not(keeps))
    def _():
        left = spread.at[pl.ds(0, kinds)]
        pltpu.make_async_copy(left, left, send_one).wait()
        got = spread.at[pl.ds(0, kinds)]
        pltpu.make_async_copy(got, got, recv_two).wait()

    def ring(index, owner, slot, peer):
        part = context.at[slot, :, pl.ds(pl.multiple_of(owner * share, LANES), share)]
        return pltpu.make_async_remote_copy(
            src_ref=part,
            dst_ref=part,
            send_sem=ring_send.at[index],
            recv_sem=ring_recv.at[index],
            device_id={"mp": peer},
            device_id_type=MESH,
        )

    up_first, up_second = ring(0, rank, 0, after), ring(1, rank, 1, after)
    down_first, down_second = ring(2, rank, 1, before), ring(3, rank, 0, before)
    up_first.start()
    down_first.start()
    up_second.start()
    down_second.start()
    up_pass, down_pass = ring(4, before, 0, after), ring(5, after, 1, before)
    up_first.wait_recv()
    up_pass.start()
    down_first.wait_recv()
    down_pass.start()
    up_second.wait_recv()
    down_second.wait_recv()
    up_pass.wait_recv()
    down_pass.wait_recv()
    for copy in (up_first, up_second, down_first, down_second, up_pass, down_pass):
        copy.wait_send()
    out_ref[...] = context[...]


def exchange(partners, past, groups, shards):
    slots, rows, width = past.shape
    kinds = slots * (rows // TILE) * (width // shards // LANES)
    return pl.pallas_call(
        functools.partial(exchange_kernel, groups, shards),
        out_shape=jax.ShapeDtypeStruct(past.shape, past.dtype),
        in_specs=[
            pl.BlockSpec(memory_space=pltpu.SMEM),
            pl.BlockSpec(memory_space=pltpu.VMEM),
        ],
        out_specs=pl.BlockSpec(memory_space=pltpu.VMEM),
        scratch_shapes=[
            pltpu.VMEM((groups, TILE, LANES), past.dtype),
            pltpu.VMEM((groups, TILE, LANES), past.dtype),
            pltpu.VMEM(past.shape, past.dtype),
            pltpu.SemaphoreType.DMA,
            pltpu.SemaphoreType.DMA,
            pltpu.SemaphoreType.DMA,
            pltpu.SemaphoreType.DMA,
            pltpu.SemaphoreType.DMA((6,)),
            pltpu.SemaphoreType.DMA((6,)),
        ],
        compiler_params=pltpu.CompilerParams(collective_id=0, has_side_effects=True),
        name="exchange",
    )(partners, past)


def laid_out(blocks, dim):
    shape = list(blocks.shape[1:])
    shape[dim] *= blocks.shape[0]
    return jnp.moveaxis(blocks, 0, dim).reshape(shape)


def sent_to_all(array, axis):
    copies = jnp.broadcast_to(array, (lax.axis_size(axis), *array.shape))
    return lax.all_to_all(copies, axis, split_axis=0, concat_axis=0, tiled=True)


def gathered_copies(array, axis, dim):
    return laid_out(sent_to_all(array, axis), dim)


def split_up(array, dim, size):
    shape = array.shape
    blocks = array.reshape(*shape[:dim], size, shape[dim] // size, *shape[dim + 1 :])
    return jnp.moveaxis(blocks, dim, 0)


def summed_on_arrival(array, axis, dim):
    blocks = split_up(array, dim, lax.axis_size(axis))
    arrived = lax.all_to_all(blocks, axis, split_axis=0, concat_axis=0, tiled=True)
    return arrived.astype(jnp.float32).sum(axis=0)


def layer_norm(values):
    center = values - jnp.mean(values, axis=-1, keepdims=True)
    spread = jnp.mean(center * center, axis=-1, keepdims=True)
    return center * lax.rsqrt(spread + 1e-06)


def body(
    current,
    past_tokens,
    counts,
    partners,
    query_weight,
    key_weight,
    value_weight,
    output_weight,
    up_weight,
    down_weight,
):
    pair_count, slot_count, model_width = current.shape
    key_count = past_tokens.shape[1]
    features = query_weight.shape[1]
    head_local = features // HEAD_DIM
    row_count = pair_count * slot_count
    shards = lax.axis_size("mp")
    share_width = model_width // shards
    column_start = lax.axis_index("mp") * share_width
    normed = layer_norm(current.astype(jnp.float32).reshape(row_count, model_width)).astype(
        jnp.bfloat16
    )
    padded = -(-key_count // TILE) * TILE
    fetched = exchange(
        partners,
        jnp.pad(past_tokens, ((0, 0), (0, padded - key_count), (0, 0))),
        lax.axis_size("pair"),
        shards,
    )[:, :key_count]
    context = layer_norm(
        fetched.astype(jnp.float32).reshape(pair_count * key_count, model_width)
    ).astype(jnp.bfloat16)
    queries = jnp.dot(normed, query_weight, preferred_element_type=jnp.float32).astype(jnp.bfloat16)
    queries = queries.reshape(pair_count, slot_count, head_local, HEAD_DIM)
    keys_local = (
        jnp.dot(context, key_weight, preferred_element_type=jnp.float32)
        .astype(jnp.bfloat16)
        .reshape(pair_count, key_count, features)
    )
    values_local = (
        jnp.dot(context, value_weight, preferred_element_type=jnp.float32)
        .astype(jnp.bfloat16)
        .reshape(pair_count, key_count, features)
    )
    key_heads = keys_local.reshape(pair_count, key_count, head_local, HEAD_DIM)
    value_heads = values_local.reshape(pair_count, key_count, head_local, HEAD_DIM)
    scores = jnp.einsum(
        "pqhd,pkhd->phqk", queries, key_heads, preferred_element_type=jnp.float32
    ) * HEAD_DIM ** (-0.5)
    row_max = jnp.max(scores, axis=-1, keepdims=True)
    lifted = jnp.exp(scores - row_max)
    weights = (lifted / jnp.sum(lifted, axis=-1, keepdims=True)).astype(jnp.bfloat16)
    attended = jnp.einsum(
        "phqk,pkhd->pqhd", weights, value_heads, preferred_element_type=jnp.float32
    ).astype(jnp.bfloat16)
    partial_value = jnp.dot(
        attended.reshape(row_count, features), output_weight, preferred_element_type=jnp.float32
    )
    current_share = lax.dynamic_slice_in_dim(
        current.reshape(row_count, model_width), column_start, share_width, 1
    ).astype(jnp.float32)
    hidden_share = current_share + lax.psum_scatter(
        partial_value, "mp", scatter_dimension=1, tiled=True
    )
    first_moment, second_moment = lax.psum(
        (jnp.sum(hidden_share, axis=1), jnp.sum(hidden_share * hidden_share, axis=1)), "mp"
    )
    row_mean = first_moment / model_width
    row_var = second_moment / model_width - row_mean * row_mean
    normed_share = (
        (hidden_share - row_mean[:, None]) * lax.rsqrt(row_var[:, None] + 1e-06)
    ).astype(jnp.bfloat16)
    mixer_in = gathered_copies(normed_share, "mp", 1)
    expanded = jax.nn.gelu(
        jnp.dot(mixer_in, up_weight, preferred_element_type=jnp.float32), approximate=False
    ).astype(jnp.bfloat16)
    mlp_result = summed_on_arrival(
        jnp.dot(expanded, down_weight, preferred_element_type=jnp.float32).astype(jnp.bfloat16),
        "mp",
        1,
    )
    is_live = (jnp.arange(slot_count, dtype=jnp.int32)[None, :] < counts[:, None]).reshape(
        row_count, 1
    )
    result = jnp.where(is_live, hidden_share + mlp_result, 0.0).astype(jnp.bfloat16)
    return result.reshape(pair_count, slot_count, share_width)


def solution(mesh):
    placed = (
        P("pair", None, None),
        P("pair", None, None),
        P("pair"),
        P(),
        P(None, "mp"),
        P(None, "mp"),
        P(None, "mp"),
        P("mp", None),
        P(None, "mp"),
        P("mp", None),
    )
    return jax.shard_map(
        body, mesh=mesh, in_specs=placed, out_specs=P("pair", None, "mp"), check_vma=False
    )
```

```python
import functools

import jax
import jax.numpy as jnp
from jax import lax
from jax.experimental import pallas as pl
from jax.experimental.pallas import tpu as pltpu
from jax.sharding import PartitionSpec as P

HEAD_DIM = 64
TILE = 16
LANES = 128
MESH = pl.DeviceIdType.MESH
F32 = jnp.float32
BF16 = jnp.bfloat16


class Ring:
    def __init__(self, part, rank, after, before, send, recv, base):
        def copy(index, owner, half, peer):
            ref = part(owner, half)
            return pltpu.make_async_remote_copy(
                src_ref=ref,
                dst_ref=ref,
                send_sem=send.at[base + index],
                recv_sem=recv.at[base + index],
                device_id={"mp": peer},
                device_id_type=MESH,
            )

        self.up = (copy(0, rank, 0, after), copy(1, rank, 1, after), copy(2, before, 0, after))
        self.down = (copy(3, rank, 1, before), copy(4, rank, 0, before), copy(5, after, 1, before))

    def start(self, step):
        self.up[step].start()
        self.down[step].start()

    def forward(self):
        self.up[0].wait_recv()
        self.up[2].start()
        self.down[0].wait_recv()
        self.down[2].start()

    def arrive(self):
        for step in (1, 2):
            self.up[step].wait_recv()
            self.down[step].wait_recv()

    def settle(self):
        for copy in self.up + self.down:
            copy.wait_send()


def normalize(source, target, rows):
    for first in range(0, rows, TILE):
        values = source[first : first + TILE, :].astype(F32)
        center = values - jnp.mean(values, axis=-1, keepdims=True)
        spread = jnp.mean(center * center, axis=-1, keepdims=True)
        target[first : first + TILE, :] = (center * lax.rsqrt(spread + 1e-06)).astype(BF16)


def gelu(values):
    return 0.5 * values * (1.0 + lax.erf(values * (0.5**0.5)))


def decoder_kernel(
    groups,
    shards,
    keys,
    partners_ref,
    past_hbm,
    current_hbm,
    query_hbm,
    key_hbm,
    value_hbm,
    output_hbm,
    up_hbm,
    down_hbm,
    out_ref,
    past,
    current,
    query_weight,
    key_weight,
    value_weight,
    output_weight,
    up_weight,
    down_weight,
    spread,
    sorted_tiles,
    context,
    normed,
    queries,
    attended,
    hidden,
    partial,
    packed,
    summed,
    landed,
    load,
    exchange_sem,
    ring_send,
    ring_recv,
):
    slots, rows, width = past.shape
    share = width // shards
    halves = share // LANES
    blocks = rows // TILE
    kinds = slots * blocks * halves
    me = lax.axis_index("pair")
    rank = lax.axis_index("mp")
    column = pl.multiple_of(rank * share, LANES)
    after = lax.rem(rank + 1, shards)
    before = lax.rem(rank + shards - 1, shards)
    across = lax.rem(rank + 2, shards)
    core = lax.rem(me, 2)
    twin = me + 1 - 2 * core

    def fetch(index, source, target):
        copy = pltpu.make_async_copy(source, target, load.at[index])
        copy.start()
        return copy

    get_output = fetch(
        0, output_hbm, output_weight.at[pl.ds(pl.multiple_of(rank * share, share), share), :]
    )
    get_past = fetch(1, past_hbm, past)
    get_current = fetch(2, current_hbm, current)
    get_query = fetch(3, query_hbm, query_weight)
    get_key = fetch(4, key_hbm, key_weight)
    get_value = fetch(5, value_hbm, value_weight)
    get_up = fetch(6, up_hbm, up_weight)
    get_down = fetch(7, down_hbm, down_weight)

    def keeper(kind):
        return (kind * groups) // kinds

    mine = (me * kinds + groups - 1) // groups
    keeps = jnp.logical_and(mine < kinds, keeper(mine) == me)

    def place(kind):
        slot = kind // (blocks * halves)
        left = kind % (blocks * halves)
        row = pl.multiple_of((left // halves) * TILE, TILE)
        lane = pl.multiple_of(column + (left % halves) * LANES, LANES)
        return slot, pl.ds(row, TILE), pl.ds(lane, LANES)

    barrier = pltpu.get_barrier_semaphore()

    def greet(step, carry):
        peer = lax.rem(me + 1 + step, groups)
        pl.semaphore_signal(barrier, inc=1, device_id={"pair": peer}, device_id_type=MESH)
        return carry

    lax.fori_loop(0, groups - 1, greet, 0)
    for peer in (after, before):
        pl.semaphore_signal(barrier, inc=1, device_id={"mp": peer}, device_id_type=MESH)
    pl.semaphore_wait(barrier, groups + 1)

    get_past.wait()
    first = (me * kinds) // groups

    def spread_one(step, carry):
        kind = lax.rem(first + step, kinds)
        target = keeper(kind)
        slot, row, lane = place(kind)

        @pl.when(target != me)
        def _():
            pltpu.make_async_remote_copy(
                src_ref=past.at[slot, row, lane],
                dst_ref=spread.at[me],
                send_sem=exchange_sem.at[0],
                recv_sem=exchange_sem.at[1],
                device_id={"pair": target},
                device_id_type=MESH,
            ).start()

        @pl.when(target == me)
        def _():
            spread[me] = past[slot, row, lane]

        return carry

    lax.fori_loop(0, kinds, spread_one, 0)

    half = share // 2
    quarter = half // 2

    def weight_rows(owner, piece):
        row = pl.multiple_of(owner * share + core * half + piece * quarter, quarter)
        return output_weight.at[pl.ds(row, quarter), :]

    weight_ring = Ring(weight_rows, rank, after, before, ring_send, ring_recv, 0)
    get_output.wait()
    weight_ring.start(0)
    weight_ring.start(1)

    get_current.wait()
    get_query.wait()
    for slot in range(slots):
        normalize(current.at[slot], normed, rows)
        queries[slot] = jnp.dot(
            normed[...], query_weight[...], preferred_element_type=F32
        ).astype(BF16)

    @pl.when(keeps)
    def _():
        slot, row, lane = place(mine)
        arrived = spread.at[pl.ds(0, groups - 1)]
        pltpu.make_async_copy(arrived, arrived, exchange_sem.at[1]).wait()

        def sort_one(step, carry):
            owner = partners_ref[step * slots + slot] // slots
            sorted_tiles[step] = spread[owner]
            return carry

        lax.fori_loop(0, groups, sort_one, 0)
        context[slot, row, lane] = sorted_tiles[me]

        def deliver(step, carry):
            target = lax.rem(me + 1 + step, groups)
            pltpu.make_async_remote_copy(
                src_ref=sorted_tiles.at[target],
                dst_ref=context.at[slot, row, lane],
                send_sem=exchange_sem.at[2],
                recv_sem=exchange_sem.at[3],
                device_id={"pair": target},
                device_id_type=MESH,
            ).start()
            return carry

        lax.fori_loop(0, groups - 1, deliver, 0)

    weight_ring.forward()

    @pl.when(keeps)
    def _():
        got = spread.at[pl.ds(0, kinds - 1)]
        pltpu.make_async_copy(got, got, exchange_sem.at[3]).wait()

    @pl.when(jnp.logical_not(keeps))
    def _():
        got = spread.at[pl.ds(0, kinds)]
        pltpu.make_async_copy(got, got, exchange_sem.at[3]).wait()

    def columns_of(buffer, slot):
        def part(owner, piece):
            lane = pl.multiple_of(owner * share + piece * LANES, LANES)
            return buffer.at[slot, :, pl.ds(lane, LANES)]

        return part

    context_rings = [
        Ring(columns_of(context, slot), rank, after, before, ring_send, ring_recv, 6 + 6 * slot)
        for slot in range(slots)
    ]
    attended_rings = [
        Ring(columns_of(attended, slot), rank, after, before, ring_send, ring_recv, 18 + 6 * slot)
        for slot in range(slots)
    ]
    context_rings[0].start(0)
    context_rings[0].start(1)
    context_rings[1].start(0)
    weight_ring.arrive()

    def to_twin(index, owner):
        row = pl.multiple_of(owner * share + core * half, half)
        ref = output_weight.at[pl.ds(row, half), :]
        return pltpu.make_async_remote_copy(
            src_ref=ref,
            dst_ref=ref,
            send_sem=ring_send.at[30 + index],
            recv_sem=ring_recv.at[30 + index],
            device_id={"pair": twin},
            device_id_type=MESH,
        )

    twins = [to_twin(index, owner) for index, owner in enumerate((before, after, across))]
    for copy in twins:
        copy.start()
    context_rings[0].forward()
    context_rings[1].start(1)

    lanes = lax.broadcasted_iota(jnp.int32, (rows, share), 1) // HEAD_DIM
    seen = lax.broadcasted_iota(jnp.int32, (rows, rows), 1) < keys

    def attend(slot):
        normalize(context.at[slot], normed, rows)
        key = jnp.dot(normed[...], key_weight[...], preferred_element_type=F32).astype(BF16)
        value = jnp.dot(normed[...], value_weight[...], preferred_element_type=F32).astype(BF16)
        query = queries[slot]
        total = jnp.zeros((rows, share), F32)
        for head in range(share // HEAD_DIM):
            one = jnp.where(lanes == head, query, jnp.zeros_like(query))
            scores = (
                lax.dot_general(one, key, (((1,), (1,)), ((), ())), preferred_element_type=F32)
                * HEAD_DIM ** (-0.5)
            )
            scores = jnp.where(seen, scores, -jnp.inf)
            lifted = jnp.exp(scores - jnp.max(scores, axis=-1, keepdims=True))
            weights = (lifted * (1.0 / jnp.sum(lifted, axis=-1, keepdims=True))).astype(BF16)
            total = jnp.where(
                lanes == head, jnp.dot(weights, value, preferred_element_type=F32), total
            )
        attended[slot, :, pl.ds(column, share)] = total.astype(BF16)

    get_key.wait()
    get_value.wait()
    context_rings[0].arrive()
    attend(0)
    attended_rings[0].start(0)
    attended_rings[0].start(1)
    context_rings[1].forward()
    context_rings[1].arrive()
    attended_rings[0].forward()
    attend(1)
    attended_rings[1].start(0)
    attended_rings[1].start(1)

    def block(owner, piece):
        return pl.ds(pl.multiple_of(owner * share + piece * LANES, LANES), LANES)

    def sends(slot):
        base = 33 + 6 * slot

        def copy(index, source, target, peer):
            return pltpu.make_async_remote_copy(
                src_ref=source,
                dst_ref=target,
                send_sem=ring_send.at[base + index],
                recv_sem=ring_recv.at[base + index],
                device_id={"mp": peer},
                device_id_type=MESH,
            )

        return [
            copy(0, packed.at[slot, :, block(across, 0)], landed.at[slot, 0], after),
            copy(1, packed.at[slot, :, block(across, 1)], landed.at[slot, 1], before),
            copy(2, packed.at[slot, :, block(after, 1)], landed.at[slot, 2], after),
            copy(3, packed.at[slot, :, block(before, 0)], landed.at[slot, 3], before),
            copy(4, summed.at[slot, 0], landed.at[slot, 4], after),
            copy(5, summed.at[slot, 1], landed.at[slot, 5], before),
        ]

    reductions = [sends(slot) for slot in range(slots)]

    def mix(slot):
        hidden[slot] = current[slot].astype(F32) + jnp.dot(
            attended[slot], output_weight[...], preferred_element_type=F32
        )
        normalize(hidden.at[slot], normed, rows)
        expanded = gelu(
            jnp.dot(normed[...], up_weight[...], preferred_element_type=F32)
        ).astype(BF16)
        result = jnp.dot(expanded, down_weight[...], preferred_element_type=F32)
        partial[slot] = result
        packed[slot] = result.astype(BF16)
        for copy in reductions[slot][:4]:
            copy.start()

    def relay(slot):
        for piece, owner in ((0, after), (1, before)):
            reductions[slot][piece].wait_recv()
            summed[slot, piece] = (
                partial[slot, :, block(owner, piece)] + landed[slot, piece].astype(F32)
            ).astype(BF16)
            reductions[slot][4 + piece].start()

    def finish(slot):
        for copy in reductions[slot][2:]:
            copy.wait_recv()
        for piece, others in ((0, (4, 3)), (1, (2, 5))):
            mine_at = block(rank, piece)
            result = partial[slot, :, mine_at]
            for other in others:
                result = result + landed[slot, other].astype(F32)
            out_ref[slot, :, piece * LANES : (piece + 1) * LANES] = (
                hidden[slot, :, mine_at] + result
            ).astype(BF16)

    attended_rings[0].arrive()
    for copy in twins:
        copy.wait_recv()
    get_up.wait()
    get_down.wait()
    attended_rings[1].forward()
    mix(0)
    attended_rings[1].arrive()
    relay(0)
    mix(1)
    finish(0)
    relay(1)
    finish(1)

    for ring in [weight_ring] + context_rings + attended_rings:
        ring.settle()
    for copy in twins + reductions[0] + reductions[1]:
        copy.wait_send()

    @pl.when(keeps)
    def _():
        left = spread.at[pl.ds(0, kinds - 1)]
        pltpu.make_async_copy(left, left, exchange_sem.at[0]).wait()
        sent = spread.at[pl.ds(0, groups - 1)]
        pltpu.make_async_copy(sent, sent, exchange_sem.at[2]).wait()

    @pl.when(jnp.logical_not(keeps))
    def _():
        left = spread.at[pl.ds(0, kinds)]
        pltpu.make_async_copy(left, left, exchange_sem.at[0]).wait()


def body(
    current,
    past_tokens,
    counts,
    partners,
    query_weight,
    key_weight,
    value_weight,
    output_weight,
    up_weight,
    down_weight,
):
    pair_count, slot_count, model_width = current.shape
    key_count = past_tokens.shape[1]
    groups, shards = lax.axis_size("pair"), lax.axis_size("mp")
    share = model_width // shards
    features = query_weight.shape[1]
    hidden_units = up_weight.shape[1]
    rows = -(-key_count // TILE) * TILE
    padding = ((0, 0), (0, rows - key_count), (0, 0))
    kinds = pair_count * (rows // TILE) * (share // LANES)
    whole = pl.BlockSpec(memory_space=pl.ANY)
    full = (pair_count, rows, model_width)
    result = pl.pallas_call(
        functools.partial(decoder_kernel, groups, shards, key_count),
        out_shape=jax.ShapeDtypeStruct((pair_count, rows, share), BF16),
        in_specs=[pl.BlockSpec(memory_space=pltpu.SMEM)] + [whole] * 8,
        out_specs=pl.BlockSpec(memory_space=pltpu.VMEM),
        scratch_shapes=[
            pltpu.VMEM(full, BF16),
            pltpu.VMEM(full, BF16),
            pltpu.VMEM((model_width, features), BF16),
            pltpu.VMEM((model_width, features), BF16),
            pltpu.VMEM((model_width, features), BF16),
            pltpu.VMEM((model_width, model_width), BF16),
            pltpu.VMEM((model_width, hidden_units), BF16),
            pltpu.VMEM((hidden_units, model_width), BF16),
            pltpu.VMEM((groups, TILE, LANES), BF16),
            pltpu.VMEM((groups, TILE, LANES), BF16),
            pltpu.VMEM(full, BF16),
            pltpu.VMEM((rows, model_width), BF16),
            pltpu.VMEM((pair_count, rows, features), BF16),
            pltpu.VMEM(full, BF16),
            pltpu.VMEM(full, F32),
            pltpu.VMEM(full, F32),
            pltpu.VMEM(full, BF16),
            pltpu.VMEM((pair_count, 2, rows, LANES), BF16),
            pltpu.VMEM((pair_count, 6, rows, LANES), BF16),
            pltpu.SemaphoreType.DMA((8,)),
            pltpu.SemaphoreType.DMA((4,)),
            pltpu.SemaphoreType.DMA((45,)),
            pltpu.SemaphoreType.DMA((45,)),
        ],
        compiler_params=pltpu.CompilerParams(
            collective_id=0, has_side_effects=True, vmem_limit_bytes=56 * 1024 * 1024
        ),
        name="decoder",
    )(
        partners,
        jnp.pad(past_tokens, padding),
        jnp.pad(current, padding),
        query_weight,
        key_weight,
        value_weight,
        output_weight,
        up_weight,
        down_weight,
    )
    live = jnp.arange(slot_count, dtype=jnp.int32)[None, :, None] < counts[:, None, None]
    return jnp.where(live, result[:, :slot_count], jnp.zeros((), BF16))


def solution(mesh):
    placed = (
        P("pair", None, None),
        P("pair", None, None),
        P("pair"),
        P(),
        P(None, "mp"),
        P(None, "mp"),
        P(None, "mp"),
        P("mp", None),
        P(None, "mp"),
        P("mp", None),
    )
    return jax.shard_map(
        body, mesh=mesh, in_specs=placed, out_specs=P("pair", None, "mp"), check_vma=False
    )
```

```python
import functools

import jax
import jax.numpy as jnp
from jax import lax
from jax.experimental import pallas as pl
from jax.experimental.pallas import tpu as pltpu
from jax.sharding import PartitionSpec as P

HEAD_DIM = 64
TILE = 16
LANES = 128
BLOCK_ROWS = 4
PIECES = 4
VMEM_LIMIT = 56 * 1024 * 1024
MESH = pl.DeviceIdType.MESH
F32 = jnp.float32
BF16 = jnp.bfloat16


class Ring:
    def __init__(self, part, rank, after, before, send, recv, base):
        def copy(index, owner, half, peer):
            ref = part(owner, half)
            return pltpu.make_async_remote_copy(
                src_ref=ref,
                dst_ref=ref,
                send_sem=send.at[base + index],
                recv_sem=recv.at[base + index],
                device_id={"mp": peer},
                device_id_type=MESH,
            )

        self.up = (copy(0, rank, 0, after), copy(1, rank, 1, after), copy(2, before, 0, after))
        self.down = (copy(3, rank, 1, before), copy(4, rank, 0, before), copy(5, after, 1, before))

    def start(self, step):
        self.up[step].start()
        self.down[step].start()

    def forward(self):
        self.up[0].wait_recv()
        self.up[2].start()
        self.down[0].wait_recv()
        self.down[2].start()

    def arrive(self):
        for step in (1, 2):
            self.up[step].wait_recv()
            self.down[step].wait_recv()

    def settle(self):
        for copy in self.up + self.down:
            copy.wait_send()


def stretches(rows, count):
    step = rows // count // TILE * TILE
    return [(k * step, rows if k == count - 1 else (k + 1) * step) for k in range(count)]


def normalized(values):
    center = values - jnp.mean(values, axis=-1, keepdims=True)
    spread = jnp.mean(center * center, axis=-1, keepdims=True)
    return (center * lax.rsqrt(spread + 1e-06)).astype(BF16)


def normalize(source, target, first, last):
    for start in range(first, last, TILE):
        stop = min(start + TILE, last)
        target[start:stop, :] = normalized(source[start:stop, :].astype(F32))


def flatten_and_normalize(source, target, first, last, kept=None):
    slots, width = source.shape[1:]
    for start in range(first, last, TILE):
        stop = min(start + TILE, last)
        tile = source[start // slots : stop // slots].reshape(stop - start, width)
        if kept is not None:
            kept[start:stop, :] = tile
        target[start:stop, :] = normalized(tile.astype(F32))


def put(target, first, last, result):
    for piece in range(target.shape[0]):
        target[piece, first:last, :] = result[:, piece * LANES : (piece + 1) * LANES]


def take(source, at):
    return jnp.concatenate([source[piece, at, :] for piece in range(source.shape[0])], axis=1)


def gelu(values):
    return 0.5 * values * (1.0 + lax.erf(values * (0.5**0.5)))


def decoder_kernel(
    groups,
    shards,
    partners_ref,
    past_hbm,
    current_hbm,
    query_hbm,
    key_hbm,
    value_hbm,
    output_hbm,
    up_hbm,
    down_hbm,
    out_ref,
    past,
    current,
    query_weight,
    key_weight,
    value_weight,
    output_weight,
    up_weight,
    down_weight,
    spread,
    sorted_tiles,
    context,
    flat,
    normed,
    queries,
    keys,
    values,
    mixed,
    attended,
    hidden,
    partial,
    packed,
    summed,
    landed,
    load,
    exchange_sem,
    ring_send,
    ring_recv,
):
    frame, slots, width = past.shape
    rows = frame * slots
    share = width // shards
    block_rows = spread.shape[1]
    kinds = frame // block_rows
    pieces = stretches(rows, PIECES)
    me = lax.axis_index("pair")
    rank = lax.axis_index("mp")
    column = pl.multiple_of(rank * share, LANES)
    after = lax.rem(rank + 1, shards)
    before = lax.rem(rank + shards - 1, shards)
    across = lax.rem(rank + 2, shards)
    core = lax.rem(me, 2)
    twin = me + 1 - 2 * core

    def fetch(index, source, target):
        copy = pltpu.make_async_copy(source, target, load.at[index])
        copy.start()
        return copy

    get_past = fetch(0, past_hbm, past)
    get_output = fetch(
        1, output_hbm, output_weight.at[pl.ds(pl.multiple_of(rank * share, share), share), :]
    )
    get_current = fetch(2, current_hbm, current)
    get_query = fetch(3, query_hbm, query_weight)
    get_key = fetch(4, key_hbm, key_weight)
    get_value = fetch(5, value_hbm, value_weight)
    get_up = fetch(6, up_hbm, up_weight)
    get_down = fetch(7, down_hbm, down_weight)

    def keeper(kind):
        return (kind * groups) // kinds

    mine = (me * kinds + groups - 1) // groups
    keeps = jnp.logical_and(mine < kinds, keeper(mine) == me)

    def place(kind):
        return pl.ds(kind * block_rows, block_rows), slice(None), pl.ds(column, share)

    barrier = pltpu.get_barrier_semaphore()

    def greet(step, carry):
        peer = lax.rem(me + 1 + step, groups)
        pl.semaphore_signal(barrier, inc=1, device_id={"pair": peer}, device_id_type=MESH)
        return carry

    lax.fori_loop(0, groups - 1, greet, 0)
    for peer in (after, before):
        pl.semaphore_signal(barrier, inc=1, device_id={"mp": peer}, device_id_type=MESH)
    pl.semaphore_wait(barrier, groups + 1)

    get_past.wait()
    first = (me * kinds) // groups

    def spread_one(step, carry):
        kind = lax.rem(first + step, kinds)
        target = keeper(kind)

        @pl.when(target != me)
        def _():
            pltpu.make_async_remote_copy(
                src_ref=past.at[place(kind)],
                dst_ref=spread.at[me],
                send_sem=exchange_sem.at[0],
                recv_sem=exchange_sem.at[1],
                device_id={"pair": target},
                device_id_type=MESH,
            ).start()

        @pl.when(target == me)
        def _():
            spread[me] = past[place(kind)]

        return carry

    lax.fori_loop(0, kinds, spread_one, 0)

    half = share // 2
    quarter = half // 2

    def weight_rows(owner, piece):
        row = pl.multiple_of(owner * share + core * half + piece * quarter, quarter)
        return output_weight.at[pl.ds(row, quarter), :]

    weight_ring = Ring(weight_rows, rank, after, before, ring_send, ring_recv, 0)
    get_output.wait()
    weight_ring.start(0)
    weight_ring.start(1)

    get_current.wait()
    get_query.wait()
    flatten_and_normalize(current, normed, 0, rows, flat)
    put(queries, 0, rows, jnp.dot(normed[...], query_weight[...], preferred_element_type=F32))

    @pl.when(keeps)
    def _():
        arrived = spread.at[pl.ds(0, groups - 1)]
        pltpu.make_async_copy(arrived, arrived, exchange_sem.at[1]).wait()
        slot = lax.broadcasted_iota(jnp.int32, spread.shape[1:], 1)

        def sort_one(step, carry):
            tile = spread[partners_ref[step * slots] // slots]
            for other in range(1, slots):
                tile = jnp.where(
                    slot == other, spread[partners_ref[step * slots + other] // slots], tile
                )
            sorted_tiles[step] = tile
            return carry

        lax.fori_loop(0, groups, sort_one, 0)
        context[place(mine)] = sorted_tiles[me]

        def deliver(step, carry):
            target = lax.rem(me + 1 + step, groups)
            pltpu.make_async_remote_copy(
                src_ref=sorted_tiles.at[target],
                dst_ref=context.at[place(mine)],
                send_sem=exchange_sem.at[2],
                recv_sem=exchange_sem.at[3],
                device_id={"pair": target},
                device_id_type=MESH,
            ).start()
            return carry

        lax.fori_loop(0, groups - 1, deliver, 0)

    weight_ring.forward()

    @pl.when(keeps)
    def _():
        got = spread.at[pl.ds(0, kinds - 1)]
        pltpu.make_async_copy(got, got, exchange_sem.at[3]).wait()

    @pl.when(jnp.logical_not(keeps))
    def _():
        got = spread.at[pl.ds(0, kinds)]
        pltpu.make_async_copy(got, got, exchange_sem.at[3]).wait()

    def lanes_of(owner, piece):
        return pl.ds(pl.multiple_of(owner * share + piece * LANES, LANES), LANES)

    def context_part(first, last):
        def part(owner, piece):
            return context.at[
                first // slots : last // slots, :, lanes_of(owner, piece)
            ]

        return part

    def attended_part(first, last):
        def part(owner, piece):
            return attended.at[first:last, lanes_of(owner, piece)]

        return part

    def rings(part, base):
        return [
            Ring(part(*piece), rank, after, before, ring_send, ring_recv, base + 6 * k)
            for k, piece in enumerate(pieces)
        ]

    context_rings = rings(context_part, 9)
    attended_rings = rings(attended_part, 9 + 6 * PIECES)
    for ring in context_rings:
        ring.start(0)
    for ring in context_rings[: PIECES // 2]:
        ring.start(1)
    weight_ring.arrive()

    def to_twin(index, owner):
        row = pl.multiple_of(owner * share + core * half, half)
        ref = output_weight.at[pl.ds(row, half), :]
        return pltpu.make_async_remote_copy(
            src_ref=ref,
            dst_ref=ref,
            send_sem=ring_send.at[6 + index],
            recv_sem=ring_recv.at[6 + index],
            device_id={"pair": twin},
            device_id_type=MESH,
        )

    twins = [to_twin(index, owner) for index, owner in enumerate((before, after, across))]
    for copy in twins:
        copy.start()
    for ring in context_rings[: PIECES // 2]:
        ring.forward()
    for ring in context_rings[PIECES // 2 :]:
        ring.start(1)
    for ring in context_rings[PIECES // 2 :]:
        ring.forward()

    get_key.wait()
    get_value.wait()
    for ring, (start, stop) in zip(context_rings, pieces):
        ring.arrive()
        flatten_and_normalize(context, normed, start, stop)
        for weight, target in ((key_weight, keys), (value_weight, values)):
            put(
                target,
                start,
                stop,
                jnp.dot(normed[start:stop, :], weight[...], preferred_element_type=F32),
            )

    heads = share // HEAD_DIM
    at_slot = [pl.ds(slot, frame, stride=slots) for slot in range(slots)]
    frame_keys = [take(keys, at).astype(BF16) for at in at_slot]
    frame_values = [take(values, at).astype(BF16) for at in at_slot]

    def attend(start, stop):
        count = -(-(stop - start) // slots // 8) * 8
        head_of = lax.broadcasted_iota(jnp.int32, (count, share), 1) // HEAD_DIM
        for slot in range(slots):
            at = pl.ds(start + slot, count, stride=slots)
            query = take(queries, at)
            stacked = jnp.concatenate(
                [jnp.where(head_of == head, query, 0.0) for head in range(heads)], axis=0
            ).astype(BF16)
            scores = (
                lax.dot_general(
                    stacked,
                    frame_keys[slot],
                    (((1,), (1,)), ((), ())),
                    preferred_element_type=F32,
                )
                * HEAD_DIM ** (-0.5)
            )
            lifted = jnp.exp(scores - jnp.max(scores, axis=-1, keepdims=True))
            weights = (lifted * (1.0 / jnp.sum(lifted, axis=-1, keepdims=True))).astype(BF16)
            spans = jnp.dot(weights, frame_values[slot], preferred_element_type=F32)
            total = spans[:count]
            for head in range(1, heads):
                total = jnp.where(head_of == head, spans[head * count : (head + 1) * count], total)
            for piece in range(mixed.shape[0]):
                mixed[piece, at, :] = total[:, piece * LANES : (piece + 1) * LANES]
        attended[start:stop, pl.ds(column, share)] = take(mixed, pl.ds(start, stop - start)).astype(
            BF16
        )

    for ring, piece in zip(attended_rings, pieces):
        attend(*piece)
        ring.start(0)
        ring.start(1)

    def sends(index, first, last):
        base = 9 + 12 * PIECES + 6 * index

        def copy(offset, source, peer):
            return pltpu.make_async_remote_copy(
                src_ref=source,
                dst_ref=landed.at[offset, first:last, :],
                send_sem=ring_send.at[base + offset],
                recv_sem=ring_recv.at[base + offset],
                device_id={"mp": peer},
                device_id_type=MESH,
            )

        return [
            copy(0, packed.at[first:last, lanes_of(across, 0)], after),
            copy(1, packed.at[first:last, lanes_of(across, 1)], before),
            copy(2, packed.at[first:last, lanes_of(after, 1)], after),
            copy(3, packed.at[first:last, lanes_of(before, 0)], before),
            copy(4, summed.at[0, first:last, :], after),
            copy(5, summed.at[1, first:last, :], before),
        ]

    reductions = [sends(index, *piece) for index, piece in enumerate(pieces)]

    def mix(index):
        first, last = pieces[index]
        hidden[first:last, :] = flat[first:last, :].astype(F32) + jnp.dot(
            attended[first:last, :], output_weight[...], preferred_element_type=F32
        )
        normalize(hidden, normed, first, last)
        expanded = gelu(
            jnp.dot(normed[first:last, :], up_weight[...], preferred_element_type=F32)
        ).astype(BF16)
        result = jnp.dot(expanded, down_weight[...], preferred_element_type=F32)
        partial[first:last, :] = result
        packed[first:last, :] = result.astype(BF16)
        for copy in reductions[index][:4]:
            copy.start()

    def relay(index):
        first, last = pieces[index]
        for piece, owner in ((0, after), (1, before)):
            reductions[index][piece].wait_recv()
            summed[piece, first:last, :] = (
                partial[first:last, lanes_of(owner, piece)]
                + landed[piece, first:last, :].astype(F32)
            ).astype(BF16)
            reductions[index][4 + piece].start()

    def finish(index):
        first, last = pieces[index]
        for copy in reductions[index][2:]:
            copy.wait_recv()
        for piece, others in ((0, (4, 3)), (1, (2, 5))):
            result = partial[first:last, lanes_of(rank, piece)]
            for other in others:
                result = result + landed[other, first:last, :].astype(F32)
            result = (hidden[first:last, lanes_of(rank, piece)] + result).astype(BF16)
            out_ref[
                first // slots : last // slots, :, piece * LANES : (piece + 1) * LANES
            ] = result.reshape((last - first) // slots, slots, LANES)

    for ring in attended_rings:
        ring.forward()
    for copy in twins:
        copy.wait_recv()
    get_up.wait()
    get_down.wait()
    for index, ring in enumerate(attended_rings):
        ring.arrive()
        mix(index)
        if index:
            relay(index - 1)
    relay(PIECES - 1)
    for index in range(PIECES):
        finish(index)

    for ring in [weight_ring] + context_rings + attended_rings:
        ring.settle()
    for copy in twins + sum(reductions, []):
        copy.wait_send()

    @pl.when(keeps)
    def _():
        left = spread.at[pl.ds(0, kinds - 1)]
        pltpu.make_async_copy(left, left, exchange_sem.at[0]).wait()
        sent = spread.at[pl.ds(0, groups - 1)]
        pltpu.make_async_copy(sent, sent, exchange_sem.at[2]).wait()

    @pl.when(jnp.logical_not(keeps))
    def _():
        left = spread.at[pl.ds(0, kinds)]
        pltpu.make_async_copy(left, left, exchange_sem.at[0]).wait()


def body(
    current,
    past_tokens,
    counts,
    partners,
    query_weight,
    key_weight,
    value_weight,
    output_weight,
    up_weight,
    down_weight,
):
    slots, frame, width = current.shape
    groups, shards = lax.axis_size("pair"), lax.axis_size("mp")
    share = width // shards
    features = query_weight.shape[1]
    hidden_units = up_weight.shape[1]
    rows = slots * frame
    spare = rows + TILE
    whole = pl.BlockSpec(memory_space=pltpu.HBM)
    packed_shape = (frame, slots, width)
    semaphores = 9 + 18 * PIECES
    result = pl.pallas_call(
        functools.partial(decoder_kernel, groups, shards),
        out_shape=jax.ShapeDtypeStruct((frame, slots, share), BF16),
        in_specs=[pl.BlockSpec(memory_space=pltpu.SMEM)] + [whole] * 8,
        out_specs=pl.BlockSpec(memory_space=pltpu.VMEM),
        scratch_shapes=[
            pltpu.VMEM(packed_shape, BF16),
            pltpu.VMEM(packed_shape, BF16),
            pltpu.VMEM((width, features), BF16),
            pltpu.VMEM((width, features), BF16),
            pltpu.VMEM((width, features), BF16),
            pltpu.VMEM((width, width), BF16),
            pltpu.VMEM((width, hidden_units), BF16),
            pltpu.VMEM((hidden_units, width), BF16),
            pltpu.VMEM((groups, BLOCK_ROWS, slots, share), BF16),
            pltpu.VMEM((groups, BLOCK_ROWS, slots, share), BF16),
            pltpu.VMEM(packed_shape, BF16),
            pltpu.VMEM((rows, width), BF16),
            pltpu.VMEM((rows, width), BF16),
            pltpu.VMEM((features // LANES, spare, LANES), F32),
            pltpu.VMEM((features // LANES, spare, LANES), F32),
            pltpu.VMEM((features // LANES, spare, LANES), F32),
            pltpu.VMEM((features // LANES, spare, LANES), F32),
            pltpu.VMEM((rows, width), BF16),
            pltpu.VMEM((rows, width), F32),
            pltpu.VMEM((rows, width), F32),
            pltpu.VMEM((rows, width), BF16),
            pltpu.VMEM((2, rows, LANES), BF16),
            pltpu.VMEM((6, rows, LANES), BF16),
            pltpu.SemaphoreType.DMA((8,)),
            pltpu.SemaphoreType.DMA((4,)),
            pltpu.SemaphoreType.DMA((semaphores,)),
            pltpu.SemaphoreType.DMA((semaphores,)),
        ],
        compiler_params=pltpu.CompilerParams(
            collective_id=0, has_side_effects=True, vmem_limit_bytes=VMEM_LIMIT
        ),
        name="decoder",
    )(
        partners,
        past_tokens.transpose(1, 0, 2),
        current.transpose(1, 0, 2),
        query_weight,
        key_weight,
        value_weight,
        output_weight,
        up_weight,
        down_weight,
    ).transpose(1, 0, 2)
    live = jnp.arange(frame, dtype=jnp.int32)[None, :, None] < counts[:, None, None]
    return jnp.where(live, result, jnp.zeros((), BF16))


def solution(mesh):
    placed = (
        P("pair", None, None),
        P("pair", None, None),
        P("pair"),
        P(),
        P(None, "mp"),
        P(None, "mp"),
        P(None, "mp"),
        P("mp", None),
        P(None, "mp"),
        P("mp", None),
    )
    return jax.shard_map(
        body, mesh=mesh, in_specs=placed, out_specs=P("pair", None, "mp"), check_vma=False
    )
```

```python
import functools
import math

import jax
import jax.numpy as jnp
from jax import lax
from jax.experimental import pallas as pl
from jax.experimental.pallas import tpu as pltpu
from jax.sharding import PartitionSpec as P

HEAD_DIM = 64
TILE = 16
LANES = 128
BLOCK_ROWS = 7
PIECES = 4
VMEM_LIMIT = 56 * 1024 * 1024
MESH = pl.DeviceIdType.MESH
F32 = jnp.float32
BF16 = jnp.bfloat16


class Ring:
    def __init__(self, part, rank, after, before, send, recv, base):
        def copy(index, owner, half, peer):
            ref = part(owner, half)
            return pltpu.make_async_remote_copy(
                src_ref=ref,
                dst_ref=ref,
                send_sem=send.at[base + index],
                recv_sem=recv.at[base + index],
                device_id={"mp": peer},
                device_id_type=MESH,
            )

        self.up = (copy(0, rank, 0, after), copy(1, rank, 1, after), copy(2, before, 0, after))
        self.down = (copy(3, rank, 1, before), copy(4, rank, 0, before), copy(5, after, 1, before))

    def start(self, step):
        self.up[step].start()
        self.down[step].start()

    def forward(self):
        self.up[0].wait_recv()
        self.up[2].start()
        self.down[0].wait_recv()
        self.down[2].start()

    def arrive(self):
        for step in (1, 2):
            self.up[step].wait_recv()
            self.down[step].wait_recv()

    def settle(self):
        for copy in self.up + self.down:
            copy.wait_send()


def stretches(rows, count):
    step = rows // count // TILE * TILE
    return [(k * step, rows if k == count - 1 else (k + 1) * step) for k in range(count)]


def normalized(values):
    center = values - jnp.mean(values, axis=-1, keepdims=True)
    spread = jnp.mean(center * center, axis=-1, keepdims=True)
    return (center * lax.rsqrt(spread + 1e-06)).astype(BF16)


def normalize(source, target, first, last):
    for start in range(first, last, TILE):
        stop = min(start + TILE, last)
        target[start:stop, :] = normalized(source[start:stop, :].astype(F32))


def flatten_and_normalize(source, target, first, last, kept=None):
    slots, width = source.shape[1:]
    for start in range(first, last, TILE):
        stop = min(start + TILE, last)
        tile = source[start // slots : stop // slots].reshape(stop - start, width)
        if kept is not None:
            kept[start:stop, :] = tile
        target[start:stop, :] = normalized(tile.astype(F32))


def put(target, first, last, result):
    for piece in range(target.shape[0]):
        target[piece, first:last, :] = result[:, piece * LANES : (piece + 1) * LANES]


def take(source, at):
    return jnp.concatenate([source[piece, at, :] for piece in range(source.shape[0])], axis=1)


def gelu(values):
    return 0.5 * values * (1.0 + lax.erf(values * (0.5**0.5)))


def decoder_kernel(
    groups,
    shards,
    partners_ref,
    counts_ref,
    past_hbm,
    current_hbm,
    query_hbm,
    key_hbm,
    value_hbm,
    output_hbm,
    up_hbm,
    down_hbm,
    out_ref,
    past,
    current,
    query_weight,
    key_weight,
    value_weight,
    output_weight,
    up_weight,
    down_weight,
    spread,
    sorted_tiles,
    context,
    flat,
    normed,
    queries,
    keys,
    values,
    mixed,
    attended,
    hidden,
    partial,
    packed,
    summed,
    landed,
    out,
    load,
    store,
    exchange_sem,
    ring_send,
    ring_recv,
):
    frame, slots, width = past.shape
    rows = frame * slots
    share = width // shards
    block_rows = spread.shape[1]
    halves = share // LANES
    kinds = frame // block_rows * halves
    side = math.isqrt(groups)
    keepers = kinds // side
    pieces = stretches(rows, PIECES)
    me = lax.axis_index("pair")
    rank = lax.axis_index("mp")
    column = pl.multiple_of(rank * share, LANES)
    after = lax.rem(rank + 1, shards)
    before = lax.rem(rank + shards - 1, shards)
    across = lax.rem(rank + 2, shards)
    core = lax.rem(me, 2)
    twin = me + 1 - 2 * core

    def fetch(index, source, target):
        copy = pltpu.make_async_copy(source, target, load.at[index])
        copy.start()
        return copy

    get_past = fetch(0, past_hbm, past)
    get_output = fetch(
        1, output_hbm, output_weight.at[pl.ds(pl.multiple_of(rank * share, share), share), :]
    )
    get_current = fetch(2, current_hbm, current)
    get_query = fetch(3, query_hbm, query_weight)
    get_key = fetch(4, key_hbm, key_weight)
    get_value = fetch(5, value_hbm, value_weight)
    get_up = fetch(6, up_hbm, up_weight)
    get_down = fetch(7, down_hbm, down_weight)

    square = me // side
    seat = lax.rem(me, side)
    keeps = seat < keepers

    def place(kind):
        lane = pl.multiple_of(column + lax.rem(kind, halves) * LANES, LANES)
        return pl.ds(kind // halves * block_rows, block_rows), slice(None), pl.ds(lane, LANES)

    def other_square(step):
        offset = (step + 1) // 2 * (1 - 2 * lax.rem(step, 2))
        return lax.rem(square + side // 2 + offset, side)

    def everyone(send):
        def one_square(step, carry):
            there = other_square(step)
            for other in range(side):
                send(there * side + other)
            return carry

        lax.fori_loop(0, side - 1, one_square, 0)
        for other in range(1, side):
            send(square * side + lax.rem(seat + other, side))

    barrier = pltpu.get_barrier_semaphore()

    def greet(peer):
        pl.semaphore_signal(barrier, inc=1, device_id={"pair": peer}, device_id_type=MESH)

    everyone(greet)
    for peer in (after, before):
        pl.semaphore_signal(barrier, inc=1, device_id={"mp": peer}, device_id_type=MESH)
    pl.semaphore_wait(barrier, groups + 1)

    get_past.wait()

    def spread_one(there, other):
        pltpu.make_async_remote_copy(
            src_ref=past.at[place(there * keepers + other)],
            dst_ref=spread.at[me],
            send_sem=exchange_sem.at[0],
            recv_sem=exchange_sem.at[1],
            device_id={"pair": there * side + other},
            device_id_type=MESH,
        ).start()

    def spread_square(step, carry):
        there = other_square(step)
        for other in range(keepers):
            spread_one(there, other)
        return carry

    lax.fori_loop(0, side - 1, spread_square, 0)
    mine = square * keepers + seat
    for other in range(keepers):
        pl.when(seat != other)(functools.partial(spread_one, square, other))

    @pl.when(keeps)
    def _():
        spread[me] = past[place(mine)]

    half = share // 2
    quarter = half // 2

    def weight_rows(owner, piece):
        row = pl.multiple_of(owner * share + core * half + piece * quarter, quarter)
        return output_weight.at[pl.ds(row, quarter), :]

    weight_ring = Ring(weight_rows, rank, after, before, ring_send, ring_recv, 0)
    get_output.wait()
    weight_ring.start(0)
    weight_ring.start(1)

    get_current.wait()
    get_query.wait()
    flatten_and_normalize(current, normed, 0, rows, flat)
    put(queries, 0, rows, jnp.dot(normed[...], query_weight[...], preferred_element_type=F32))

    @pl.when(keeps)
    def _():
        arrived = spread.at[pl.ds(0, groups - 1)]
        pltpu.make_async_copy(arrived, arrived, exchange_sem.at[1]).wait()
        slot = lax.broadcasted_iota(jnp.int32, spread.shape[1:], 1)

        def sort_one(step, carry):
            tile = spread[partners_ref[step * slots] // slots]
            for other in range(1, slots):
                tile = jnp.where(
                    slot == other, spread[partners_ref[step * slots + other] // slots], tile
                )
            sorted_tiles[step] = tile
            return carry

        lax.fori_loop(0, groups, sort_one, 0, unroll=8)
        context[place(mine)] = sorted_tiles[me]

        def deliver(target):
            pltpu.make_async_remote_copy(
                src_ref=sorted_tiles.at[target],
                dst_ref=context.at[place(mine)],
                send_sem=exchange_sem.at[2],
                recv_sem=exchange_sem.at[3],
                device_id={"pair": target},
                device_id_type=MESH,
            ).start()

        everyone(deliver)

    weight_ring.forward()

    @pl.when(keeps)
    def _():
        got = spread.at[pl.ds(0, kinds - 1)]
        pltpu.make_async_copy(got, got, exchange_sem.at[3]).wait()

    @pl.when(jnp.logical_not(keeps))
    def _():
        got = spread.at[pl.ds(0, kinds)]
        pltpu.make_async_copy(got, got, exchange_sem.at[3]).wait()

    def lanes_of(owner, piece):
        return pl.ds(pl.multiple_of(owner * share + piece * LANES, LANES), LANES)

    def context_part(first, last):
        def part(owner, piece):
            return context.at[
                first // slots : last // slots, :, lanes_of(owner, piece)
            ]

        return part

    def attended_part(first, last):
        def part(owner, piece):
            return attended.at[first:last, lanes_of(owner, piece)]

        return part

    def rings(part, base):
        return [
            Ring(part(*piece), rank, after, before, ring_send, ring_recv, base + 6 * k)
            for k, piece in enumerate(pieces)
        ]

    context_rings = rings(context_part, 9)
    attended_rings = rings(attended_part, 9 + 6 * PIECES)
    for ring in context_rings:
        ring.start(0)
    for ring in context_rings[: PIECES // 2]:
        ring.start(1)
    weight_ring.arrive()

    def to_twin(index, owner):
        row = pl.multiple_of(owner * share + core * half, half)
        ref = output_weight.at[pl.ds(row, half), :]
        return pltpu.make_async_remote_copy(
            src_ref=ref,
            dst_ref=ref,
            send_sem=ring_send.at[6 + index],
            recv_sem=ring_recv.at[6 + index],
            device_id={"pair": twin},
            device_id_type=MESH,
        )

    twins = [to_twin(index, owner) for index, owner in enumerate((before, after, across))]
    for copy in twins:
        copy.start()
    for ring in context_rings[: PIECES // 2]:
        ring.forward()
    for ring in context_rings[PIECES // 2 :]:
        ring.start(1)
    for ring in context_rings[PIECES // 2 :]:
        ring.forward()

    get_key.wait()
    get_value.wait()
    for ring, (start, stop) in zip(context_rings, pieces):
        ring.arrive()
        flatten_and_normalize(context, normed, start, stop)
        for weight, target in ((key_weight, keys), (value_weight, values)):
            put(
                target,
                start,
                stop,
                jnp.dot(normed[start:stop, :], weight[...], preferred_element_type=F32),
            )

    heads = share // HEAD_DIM
    at_slot = [pl.ds(slot, frame, stride=slots) for slot in range(slots)]
    frame_keys = [take(keys, at).astype(BF16) for at in at_slot]
    frame_values = [take(values, at).astype(BF16) for at in at_slot]

    def attend(start, stop):
        count = -(-(stop - start) // slots // 8) * 8
        head_of = lax.broadcasted_iota(jnp.int32, (count, share), 1) // HEAD_DIM
        for slot in range(slots):
            at = pl.ds(start + slot, count, stride=slots)
            query = take(queries, at)
            stacked = jnp.concatenate(
                [jnp.where(head_of == head, query, 0.0) for head in range(heads)], axis=0
            ).astype(BF16)
            scores = (
                lax.dot_general(
                    stacked,
                    frame_keys[slot],
                    (((1,), (1,)), ((), ())),
                    preferred_element_type=F32,
                )
                * HEAD_DIM ** (-0.5)
            )
            lifted = jnp.exp(scores - jnp.max(scores, axis=-1, keepdims=True))
            weights = (lifted * (1.0 / jnp.sum(lifted, axis=-1, keepdims=True))).astype(BF16)
            spans = jnp.dot(weights, frame_values[slot], preferred_element_type=F32)
            total = spans[:count]
            for head in range(1, heads):
                total = jnp.where(head_of == head, spans[head * count : (head + 1) * count], total)
            for piece in range(mixed.shape[0]):
                mixed[piece, at, :] = total[:, piece * LANES : (piece + 1) * LANES]
        attended[start:stop, pl.ds(column, share)] = take(mixed, pl.ds(start, stop - start)).astype(
            BF16
        )

    def launch(ring):
        ring.start(0)
        ring.start(1)

    for index, piece in enumerate(pieces):
        attend(*piece)
        if index < 2:
            launch(attended_rings[index])

    def sends(index, first, last):
        base = 9 + 12 * PIECES + 6 * index

        def copy(offset, source, peer):
            return pltpu.make_async_remote_copy(
                src_ref=source,
                dst_ref=landed.at[offset, first:last, :],
                send_sem=ring_send.at[base + offset],
                recv_sem=ring_recv.at[base + offset],
                device_id={"mp": peer},
                device_id_type=MESH,
            )

        return [
            copy(0, packed.at[first:last, lanes_of(across, 0)], after),
            copy(1, packed.at[first:last, lanes_of(across, 1)], before),
            copy(2, packed.at[first:last, lanes_of(after, 1)], after),
            copy(3, packed.at[first:last, lanes_of(before, 0)], before),
            copy(4, summed.at[0, first:last, :], after),
            copy(5, summed.at[1, first:last, :], before),
        ]

    reductions = [sends(index, *piece) for index, piece in enumerate(pieces)]

    def mix(index):
        first, last = pieces[index]
        hidden[first:last, :] = flat[first:last, :].astype(F32) + jnp.dot(
            attended[first:last, :], output_weight[...], preferred_element_type=F32
        )
        normalize(hidden, normed, first, last)
        expanded = gelu(
            jnp.dot(normed[first:last, :], up_weight[...], preferred_element_type=F32)
        ).astype(BF16)
        result = jnp.dot(expanded, down_weight[...], preferred_element_type=F32)
        partial[first:last, :] = result
        packed[first:last, :] = result.astype(BF16)
        for copy in reductions[index][:4]:
            copy.start()

    def relay(index):
        first, last = pieces[index]
        for piece, owner in ((0, after), (1, before)):
            reductions[index][piece].wait_recv()
            summed[piece, first:last, :] = (
                partial[first:last, lanes_of(owner, piece)]
                + landed[piece, first:last, :].astype(F32)
            ).astype(BF16)
            reductions[index][4 + piece].start()

    def finish(index):
        first, last = pieces[index]
        for copy in reductions[index][2:]:
            copy.wait_recv()
        for piece, others in ((0, (4, 3)), (1, (2, 5))):
            result = partial[first:last, lanes_of(rank, piece)]
            for other in others:
                result = result + landed[other, first:last, :].astype(F32)
            row = first + lax.broadcasted_iota(jnp.int32, result.shape, 0)
            limit = counts_ref[0]
            for slot in range(1, slots):
                limit = jnp.where(lax.rem(row, slots) == slot, counts_ref[slot], limit)
            result = hidden[first:last, lanes_of(rank, piece)] + result
            result = jnp.where(row // slots < limit, result, 0.0).astype(BF16)
            out[
                first // slots : last // slots, :, piece * LANES : (piece + 1) * LANES
            ] = result.reshape((last - first) // slots, slots, LANES)
        at = slice(first // slots, last // slots)
        pltpu.make_async_copy(out.at[at], out_ref.at[at], store.at[index]).start()

    attended_rings[0].forward()
    launch(attended_rings[2])
    attended_rings[1].forward()
    launch(attended_rings[3])
    attended_rings[2].forward()
    for copy in twins:
        copy.wait_recv()
    get_up.wait()
    get_down.wait()
    for index, ring in enumerate(attended_rings):
        ring.arrive()
        mix(index)
        if index == 0:
            attended_rings[3].forward()
        else:
            relay(index - 1)
    finish(0)
    relay(PIECES - 1)
    for index in range(1, PIECES):
        finish(index)

    for index, (first, last) in enumerate(pieces):
        at = slice(first // slots, last // slots)
        pltpu.make_async_copy(out.at[at], out_ref.at[at], store.at[index]).wait()
    for ring in [weight_ring] + context_rings + attended_rings:
        ring.settle()
    for copy in twins + sum(reductions, []):
        copy.wait_send()

    @pl.when(keeps)
    def _():
        left = spread.at[pl.ds(0, kinds - 1)]
        pltpu.make_async_copy(left, left, exchange_sem.at[0]).wait()
        sent = spread.at[pl.ds(0, groups - 1)]
        pltpu.make_async_copy(sent, sent, exchange_sem.at[2]).wait()

    @pl.when(jnp.logical_not(keeps))
    def _():
        left = spread.at[pl.ds(0, kinds)]
        pltpu.make_async_copy(left, left, exchange_sem.at[0]).wait()


def body(
    current,
    past_tokens,
    counts,
    partners,
    query_weight,
    key_weight,
    value_weight,
    output_weight,
    up_weight,
    down_weight,
):
    slots, frame, width = current.shape
    groups, shards = lax.axis_size("pair"), lax.axis_size("mp")
    share = width // shards
    features = query_weight.shape[1]
    hidden_units = up_weight.shape[1]
    rows = slots * frame
    spare = rows + TILE
    whole = pl.BlockSpec(memory_space=pltpu.HBM)
    packed_shape = (frame, slots, width)
    semaphores = 9 + 18 * PIECES
    return pl.pallas_call(
        functools.partial(decoder_kernel, groups, shards),
        out_shape=jax.ShapeDtypeStruct((frame, slots, share), BF16),
        in_specs=[pl.BlockSpec(memory_space=pltpu.SMEM)] * 2 + [whole] * 8,
        out_specs=whole,
        scratch_shapes=[
            pltpu.VMEM(packed_shape, BF16),
            pltpu.VMEM(packed_shape, BF16),
            pltpu.VMEM((width, features), BF16),
            pltpu.VMEM((width, features), BF16),
            pltpu.VMEM((width, features), BF16),
            pltpu.VMEM((width, width), BF16),
            pltpu.VMEM((width, hidden_units), BF16),
            pltpu.VMEM((hidden_units, width), BF16),
            pltpu.VMEM((groups, BLOCK_ROWS, slots, LANES), BF16),
            pltpu.VMEM((groups, BLOCK_ROWS, slots, LANES), BF16),
            pltpu.VMEM(packed_shape, BF16),
            pltpu.VMEM((rows, width), BF16),
            pltpu.VMEM((rows, width), BF16),
            pltpu.VMEM((features // LANES, spare, LANES), F32),
            pltpu.VMEM((features // LANES, spare, LANES), F32),
            pltpu.VMEM((features // LANES, spare, LANES), F32),
            pltpu.VMEM((features // LANES, spare, LANES), F32),
            pltpu.VMEM((rows, width), BF16),
            pltpu.VMEM((rows, width), F32),
            pltpu.VMEM((rows, width), F32),
            pltpu.VMEM((rows, width), BF16),
            pltpu.VMEM((2, rows, LANES), BF16),
            pltpu.VMEM((6, rows, LANES), BF16),
            pltpu.VMEM((frame, slots, share), BF16),
            pltpu.SemaphoreType.DMA((8,)),
            pltpu.SemaphoreType.DMA((PIECES,)),
            pltpu.SemaphoreType.DMA((4,)),
            pltpu.SemaphoreType.DMA((semaphores,)),
            pltpu.SemaphoreType.DMA((semaphores,)),
        ],
        compiler_params=pltpu.CompilerParams(
            collective_id=0, has_side_effects=True, vmem_limit_bytes=VMEM_LIMIT
        ),
        name="decoder",
    )(
        partners,
        counts,
        past_tokens.transpose(1, 0, 2),
        current.transpose(1, 0, 2),
        query_weight,
        key_weight,
        value_weight,
        output_weight,
        up_weight,
        down_weight,
    ).transpose(1, 0, 2)


def solution(mesh):
    placed = (
        P("pair", None, None),
        P("pair", None, None),
        P("pair"),
        P(),
        P(None, "mp"),
        P(None, "mp"),
        P(None, "mp"),
        P("mp", None),
        P(None, "mp"),
        P("mp", None),
    )
    return jax.shard_map(
        body, mesh=mesh, in_specs=placed, out_specs=P("pair", None, "mp"), check_vma=False
    )
```

```python
import functools
import math

import jax
import jax.numpy as jnp
from jax import lax
from jax.experimental import pallas as pl
from jax.experimental.pallas import tpu as pltpu
from jax.sharding import PartitionSpec as P

HEAD_DIM = 64
TILE = 16
LANES = 128
BLOCK_ROWS = 7
PIECES = 4
VMEM_LIMIT = 56 * 1024 * 1024
MESH = pl.DeviceIdType.MESH
F32 = jnp.float32
BF16 = jnp.bfloat16


class Ring:
    def __init__(self, part, rank, after, before, send, recv, base):
        def copy(index, owner, half, peer):
            ref = part(owner, half)
            return pltpu.make_async_remote_copy(
                src_ref=ref,
                dst_ref=ref,
                send_sem=send.at[base + index],
                recv_sem=recv.at[base + index],
                device_id={"mp": peer},
                device_id_type=MESH,
            )

        self.up = (copy(0, rank, 0, after), copy(1, rank, 1, after), copy(2, before, 0, after))
        self.down = (copy(3, rank, 1, before), copy(4, rank, 0, before), copy(5, after, 1, before))

    def start(self, step):
        self.up[step].start()
        self.down[step].start()

    def forward(self):
        self.up[0].wait_recv()
        self.up[2].start()
        self.down[0].wait_recv()
        self.down[2].start()

    def arrive(self):
        for step in (1, 2):
            self.up[step].wait_recv()
            self.down[step].wait_recv()

    def settle(self):
        for copy in self.up + self.down:
            copy.wait_send()


def stretches(rows, count):
    step = rows // count // TILE * TILE
    return [(k * step, rows if k == count - 1 else (k + 1) * step) for k in range(count)]


def normalized(values):
    center = values - jnp.mean(values, axis=-1, keepdims=True)
    spread = jnp.mean(center * center, axis=-1, keepdims=True)
    return (center * lax.rsqrt(spread + 1e-06)).astype(BF16)


def normalize(source, target, first, last):
    for start in range(first, last, TILE):
        stop = min(start + TILE, last)
        target[start:stop, :] = normalized(source[start:stop, :].astype(F32))


def flatten_and_normalize(source, target, first, last, kept=None):
    slots, width = source.shape[1:]
    for start in range(first, last, TILE):
        stop = min(start + TILE, last)
        tile = source[start // slots : stop // slots].reshape(stop - start, width)
        if kept is not None:
            kept[start:stop, :] = tile
        target[start:stop, :] = normalized(tile.astype(F32))


def put(target, first, last, result):
    for piece in range(target.shape[0]):
        target[piece, first:last, :] = result[:, piece * LANES : (piece + 1) * LANES]


def take(source, at):
    return jnp.concatenate([source[piece, at, :] for piece in range(source.shape[0])], axis=1)


def gelu(values):
    return 0.5 * values * (1.0 + lax.erf(values * (0.5**0.5)))


def decoder_kernel(
    groups,
    shards,
    partners_ref,
    counts_ref,
    past_hbm,
    current_hbm,
    query_hbm,
    key_hbm,
    value_hbm,
    output_hbm,
    up_hbm,
    down_hbm,
    out_ref,
    past,
    current,
    query_weight,
    key_weight,
    value_weight,
    output_weight,
    up_weight,
    down_weight,
    spread,
    sorted_tiles,
    context,
    flat,
    normed,
    queries,
    keys,
    values,
    mixed,
    attended,
    hidden,
    partial,
    packed,
    summed,
    landed,
    out,
    load,
    store,
    exchange_sem,
    ring_send,
    ring_recv,
):
    frame, slots, width = past.shape
    rows = frame * slots
    share = width // shards
    block_rows = spread.shape[1]
    halves = share // LANES
    kinds = frame // block_rows * halves
    side = math.isqrt(groups)
    keepers = kinds // side
    pieces = stretches(rows, PIECES)
    me = lax.axis_index("pair")
    rank = lax.axis_index("mp")
    column = pl.multiple_of(rank * share, LANES)
    after = lax.rem(rank + 1, shards)
    before = lax.rem(rank + shards - 1, shards)
    across = lax.rem(rank + 2, shards)
    core = lax.rem(me, 2)
    twin = me + 1 - 2 * core

    def fetch(index, source, target):
        copy = pltpu.make_async_copy(source, target, load.at[index])
        copy.start()
        return copy

    get_past = fetch(0, past_hbm, past)
    get_output = fetch(
        1, output_hbm, output_weight.at[pl.ds(pl.multiple_of(rank * share, share), share), :]
    )
    get_current = fetch(2, current_hbm, current)
    get_query = fetch(3, query_hbm, query_weight)
    get_key = fetch(4, key_hbm, key_weight)
    get_value = fetch(5, value_hbm, value_weight)
    get_up = fetch(6, up_hbm, up_weight)
    get_down = fetch(7, down_hbm, down_weight)

    square = me // side
    seat = lax.rem(me, side)
    keeps = seat < keepers

    def place(kind):
        lane = pl.multiple_of(column + lax.rem(kind, halves) * LANES, LANES)
        return pl.ds(kind // halves * block_rows, block_rows), slice(None), pl.ds(lane, LANES)

    def other_square(step):
        offset = (step + 1) // 2 * (1 - 2 * lax.rem(step, 2))
        return lax.rem(square + side // 2 + offset, side)

    group = side // 2
    part = square // group
    corner = lax.rem(square, group)
    frame_part = frame // 2

    def own_half_first(send):
        for step in (2, 1, 3):
            there = part * group + lax.rem(corner + step, group)
            for other in range(side):
                send(there * side + other)
        for other in range(1, side):
            send(square * side + lax.rem(seat + other, side))
        for step in (0, 1, 3, 2):
            there = (1 - part) * group + lax.rem(corner + step, group)
            for other in range(side):
                send(there * side + other)

    def everyone(send):
        def one_square(step, carry):
            there = other_square(step)
            for other in range(side):
                send(there * side + other)
            return carry

        lax.fori_loop(0, side - 1, one_square, 0)
        for other in range(1, side):
            send(square * side + lax.rem(seat + other, side))

    barrier = pltpu.get_barrier_semaphore()

    def greet(peer):
        pl.semaphore_signal(barrier, inc=1, device_id={"pair": peer}, device_id_type=MESH)

    everyone(greet)
    for peer in (after, before):
        pl.semaphore_signal(barrier, inc=1, device_id={"mp": peer}, device_id_type=MESH)
    pl.semaphore_wait(barrier, groups + 1)

    get_past.wait()

    def spread_one(there, other):
        pltpu.make_async_remote_copy(
            src_ref=past.at[place(there * keepers + other)],
            dst_ref=spread.at[me],
            send_sem=exchange_sem.at[0],
            recv_sem=exchange_sem.at[1],
            device_id={"pair": there * side + other},
            device_id_type=MESH,
        ).start()

    def spread_square(step, carry):
        there = other_square(step)
        for other in range(keepers):
            spread_one(there, other)
        return carry

    lax.fori_loop(0, side - 1, spread_square, 0)
    mine = square * keepers + seat
    for other in range(keepers):
        pl.when(seat != other)(functools.partial(spread_one, square, other))

    @pl.when(keeps)
    def _():
        spread[me] = past[place(mine)]

    half = share // 2
    quarter = half // 2

    def weight_rows(owner, piece):
        row = pl.multiple_of(owner * share + core * half + piece * quarter, quarter)
        return output_weight.at[pl.ds(row, quarter), :]

    weight_ring = Ring(weight_rows, rank, after, before, ring_send, ring_recv, 0)
    get_output.wait()
    weight_ring.start(0)
    weight_ring.start(1)

    get_current.wait()
    get_query.wait()
    flatten_and_normalize(current, normed, 0, rows, flat)
    put(
        queries, 0, rows, jnp.dot(normed[0:rows, :], query_weight[...], preferred_element_type=F32)
    )

    @pl.when(keeps)
    def _():
        arrived = spread.at[pl.ds(0, groups - 1)]
        pltpu.make_async_copy(arrived, arrived, exchange_sem.at[1]).wait()
        slot = lax.broadcasted_iota(jnp.int32, spread.shape[1:], 1)

        def sort_one(step, carry):
            tile = spread[partners_ref[step * slots] // slots]
            for other in range(1, slots):
                tile = jnp.where(
                    slot == other, spread[partners_ref[step * slots + other] // slots], tile
                )
            sorted_tiles[step] = tile
            return carry

        lax.fori_loop(0, groups, sort_one, 0, unroll=8)
        context[place(mine)] = sorted_tiles[me]

        def deliver(target):
            pltpu.make_async_remote_copy(
                src_ref=sorted_tiles.at[target],
                dst_ref=context.at[place(mine)],
                send_sem=exchange_sem.at[2],
                recv_sem=exchange_sem.at[3 + part],
                device_id={"pair": target},
                device_id_type=MESH,
            ).start()

        own_half_first(deliver)

    weight_ring.forward()

    @pl.when(keeps)
    def _():
        got = spread.at[pl.ds(0, kinds // 2 - 1)]
        pltpu.make_async_copy(got, got, exchange_sem.at[3 + part]).wait()

    @pl.when(jnp.logical_not(keeps))
    def _():
        got = spread.at[pl.ds(0, kinds // 2)]
        pltpu.make_async_copy(got, got, exchange_sem.at[3 + part]).wait()

    def lanes_of(owner, piece):
        return pl.ds(pl.multiple_of(owner * share + piece * LANES, LANES), LANES)

    def context_part(index):
        size = frame_part // 2
        start = (part if index < 2 else 1 - part) * frame_part + index % 2 * size

        def of(owner, piece):
            return context.at[pl.ds(start, size), :, lanes_of(owner, piece)]

        return of

    def attended_part(first, last):
        def part(owner, piece):
            return attended.at[first:last, lanes_of(owner, piece)]

        return part

    def make_ring(of, base):
        return Ring(of, rank, after, before, ring_send, ring_recv, base)

    context_rings = [make_ring(context_part(k), 9 + 6 * k) for k in range(4)]
    attended_rings = [
        make_ring(attended_part(*piece), 33 + 6 * k) for k, piece in enumerate(pieces)
    ]

    def launch(ring):
        ring.start(0)
        ring.start(1)

    for ring in context_rings[:2]:
        ring.start(0)
    for ring in context_rings[:2]:
        ring.start(1)
    weight_ring.arrive()

    def to_twin(index, owner):
        row = pl.multiple_of(owner * share + core * half, half)
        ref = output_weight.at[pl.ds(row, half), :]
        return pltpu.make_async_remote_copy(
            src_ref=ref,
            dst_ref=ref,
            send_sem=ring_send.at[6 + index],
            recv_sem=ring_recv.at[6 + index],
            device_id={"pair": twin},
            device_id_type=MESH,
        )

    twins = [to_twin(index, owner) for index, owner in enumerate((before, after, across))]
    for copy in twins:
        copy.start()
    for ring in context_rings[:2]:
        ring.forward()
    got = spread.at[pl.ds(0, kinds // 2)]
    pltpu.make_async_copy(got, got, exchange_sem.at[3 + 1 - part]).wait()
    for ring in context_rings[2:]:
        ring.start(0)
    for ring in context_rings[2:]:
        ring.start(1)

    get_key.wait()
    get_value.wait()
    part_rows = frame_part * slots

    def project(index):
        at = part if index == 0 else 1 - part
        base = index * (normed.shape[0] // 2)
        for start in range(0, part_rows, TILE):
            count = min(TILE, part_rows - start)
            tile = context[pl.ds(at * frame_part + start // slots, count // slots)]
            normed[base + start : base + start + count, :] = normalized(
                tile.reshape(count, width).astype(F32)
            )
        for weight, target in ((key_weight, keys), (value_weight, values)):
            result = jnp.dot(
                normed[base : base + part_rows, :], weight[...], preferred_element_type=F32
            )
            for piece in range(halves):
                target[at, piece, 0:part_rows, :] = result[:, piece * LANES : (piece + 1) * LANES]

    for index in range(2):
        for ring in context_rings[2 * index : 2 * index + 2]:
            if index:
                ring.forward()
        for ring in context_rings[2 * index : 2 * index + 2]:
            ring.arrive()
        project(index)

    heads = share // HEAD_DIM

    def of_slot(source, slot):
        at = pl.ds(slot, frame_part, stride=slots)
        return jnp.concatenate([take(source.at[k], at) for k in range(2)], axis=0).astype(BF16)

    frame_keys = [of_slot(keys, slot) for slot in range(slots)]
    frame_values = [of_slot(values, slot) for slot in range(slots)]

    def attend(start, stop):
        count = -(-(stop - start) // slots // 8) * 8
        head_of = lax.broadcasted_iota(jnp.int32, (count, share), 1) // HEAD_DIM
        for slot in range(slots):
            at = pl.ds(start + slot, count, stride=slots)
            query = take(queries, at)
            stacked = jnp.concatenate(
                [jnp.where(head_of == head, query, 0.0) for head in range(heads)], axis=0
            ).astype(BF16)
            scores = (
                lax.dot_general(
                    stacked,
                    frame_keys[slot],
                    (((1,), (1,)), ((), ())),
                    preferred_element_type=F32,
                )
                * HEAD_DIM ** (-0.5)
            )
            lifted = jnp.exp(scores - jnp.max(scores, axis=-1, keepdims=True))
            weights = (lifted * (1.0 / jnp.sum(lifted, axis=-1, keepdims=True))).astype(BF16)
            spans = jnp.dot(weights, frame_values[slot], preferred_element_type=F32)
            total = spans[:count]
            for head in range(1, heads):
                total = jnp.where(head_of == head, spans[head * count : (head + 1) * count], total)
            for piece in range(mixed.shape[0]):
                mixed[piece, at, :] = total[:, piece * LANES : (piece + 1) * LANES]
        attended[start:stop, pl.ds(column, share)] = take(mixed, pl.ds(start, stop - start)).astype(
            BF16
        )

    for index, piece in enumerate(pieces):
        attend(*piece)
        if index < 2:
            launch(attended_rings[index])

    def sends(index, first, last):
        base = 33 + 6 * PIECES + 6 * index

        def copy(offset, source, peer):
            return pltpu.make_async_remote_copy(
                src_ref=source,
                dst_ref=landed.at[offset, first:last, :],
                send_sem=ring_send.at[base + offset],
                recv_sem=ring_recv.at[base + offset],
                device_id={"mp": peer},
                device_id_type=MESH,
            )

        return [
            copy(0, packed.at[first:last, lanes_of(across, 0)], after),
            copy(1, packed.at[first:last, lanes_of(across, 1)], before),
            copy(2, packed.at[first:last, lanes_of(after, 1)], after),
            copy(3, packed.at[first:last, lanes_of(before, 0)], before),
            copy(4, summed.at[0, first:last, :], after),
            copy(5, summed.at[1, first:last, :], before),
        ]

    reductions = [sends(index, *piece) for index, piece in enumerate(pieces)]

    def mix(index):
        first, last = pieces[index]
        hidden[first:last, :] = flat[first:last, :].astype(F32) + jnp.dot(
            attended[first:last, :], output_weight[...], preferred_element_type=F32
        )
        normalize(hidden, normed, first, last)
        expanded = gelu(
            jnp.dot(normed[first:last, :], up_weight[...], preferred_element_type=F32)
        ).astype(BF16)
        result = jnp.dot(expanded, down_weight[...], preferred_element_type=F32)
        partial[first:last, :] = result
        packed[first:last, :] = result.astype(BF16)
        for copy in reductions[index][:4]:
            copy.start()

    def relay(index):
        first, last = pieces[index]
        for piece, owner in ((0, after), (1, before)):
            reductions[index][piece].wait_recv()
            summed[piece, first:last, :] = (
                partial[first:last, lanes_of(owner, piece)]
                + landed[piece, first:last, :].astype(F32)
            ).astype(BF16)
            reductions[index][4 + piece].start()

    def finish(index):
        first, last = pieces[index]
        for copy in reductions[index][2:]:
            copy.wait_recv()
        for piece, others in ((0, (4, 3)), (1, (2, 5))):
            result = partial[first:last, lanes_of(rank, piece)]
            for other in others:
                result = result + landed[other, first:last, :].astype(F32)
            row = first + lax.broadcasted_iota(jnp.int32, result.shape, 0)
            limit = counts_ref[0]
            for slot in range(1, slots):
                limit = jnp.where(lax.rem(row, slots) == slot, counts_ref[slot], limit)
            result = hidden[first:last, lanes_of(rank, piece)] + result
            result = jnp.where(row // slots < limit, result, 0.0).astype(BF16)
            out[
                first // slots : last // slots, :, piece * LANES : (piece + 1) * LANES
            ] = result.reshape((last - first) // slots, slots, LANES)
        at = slice(first // slots, last // slots)
        pltpu.make_async_copy(out.at[at], out_ref.at[at], store.at[index]).start()

    attended_rings[0].forward()
    launch(attended_rings[2])
    attended_rings[1].forward()
    launch(attended_rings[3])
    attended_rings[2].forward()
    for copy in twins:
        copy.wait_recv()
    get_up.wait()
    get_down.wait()
    for index, ring in enumerate(attended_rings):
        ring.arrive()
        mix(index)
        if index == 0:
            attended_rings[3].forward()
        else:
            relay(index - 1)
    finish(0)
    relay(PIECES - 1)
    for index in range(1, PIECES):
        finish(index)

    for index, (first, last) in enumerate(pieces):
        at = slice(first // slots, last // slots)
        pltpu.make_async_copy(out.at[at], out_ref.at[at], store.at[index]).wait()
    for ring in [weight_ring] + context_rings + attended_rings:
        ring.settle()
    for copy in twins + sum(reductions, []):
        copy.wait_send()

    @pl.when(keeps)
    def _():
        left = spread.at[pl.ds(0, kinds - 1)]
        pltpu.make_async_copy(left, left, exchange_sem.at[0]).wait()
        sent = spread.at[pl.ds(0, groups - 1)]
        pltpu.make_async_copy(sent, sent, exchange_sem.at[2]).wait()

    @pl.when(jnp.logical_not(keeps))
    def _():
        left = spread.at[pl.ds(0, kinds)]
        pltpu.make_async_copy(left, left, exchange_sem.at[0]).wait()


def body(
    current,
    past_tokens,
    counts,
    partners,
    query_weight,
    key_weight,
    value_weight,
    output_weight,
    up_weight,
    down_weight,
):
    slots, frame, width = current.shape
    groups, shards = lax.axis_size("pair"), lax.axis_size("mp")
    share = width // shards
    features = query_weight.shape[1]
    hidden_units = up_weight.shape[1]
    rows = slots * frame
    spare = rows + TILE
    half_rows = -(-rows // 2 // TILE) * TILE
    whole = pl.BlockSpec(memory_space=pltpu.HBM)
    packed_shape = (frame, slots, width)
    semaphores = 33 + 12 * PIECES
    return pl.pallas_call(
        functools.partial(decoder_kernel, groups, shards),
        out_shape=jax.ShapeDtypeStruct((frame, slots, share), BF16),
        in_specs=[pl.BlockSpec(memory_space=pltpu.SMEM)] * 2 + [whole] * 8,
        out_specs=whole,
        scratch_shapes=[
            pltpu.VMEM(packed_shape, BF16),
            pltpu.VMEM(packed_shape, BF16),
            pltpu.VMEM((width, features), BF16),
            pltpu.VMEM((width, features), BF16),
            pltpu.VMEM((width, features), BF16),
            pltpu.VMEM((width, width), BF16),
            pltpu.VMEM((width, hidden_units), BF16),
            pltpu.VMEM((hidden_units, width), BF16),
            pltpu.VMEM((groups, BLOCK_ROWS, slots, LANES), BF16),
            pltpu.VMEM((groups, BLOCK_ROWS, slots, LANES), BF16),
            pltpu.VMEM(packed_shape, BF16),
            pltpu.VMEM((rows, width), BF16),
            pltpu.VMEM((2 * half_rows, width), BF16),
            pltpu.VMEM((features // LANES, spare, LANES), F32),
            pltpu.VMEM((2, features // LANES, half_rows, LANES), F32),
            pltpu.VMEM((2, features // LANES, half_rows, LANES), F32),
            pltpu.VMEM((features // LANES, spare, LANES), F32),
            pltpu.VMEM((rows, width), BF16),
            pltpu.VMEM((rows, width), F32),
            pltpu.VMEM((rows, width), F32),
            pltpu.VMEM((rows, width), BF16),
            pltpu.VMEM((2, rows, LANES), BF16),
            pltpu.VMEM((6, rows, LANES), BF16),
            pltpu.VMEM((frame, slots, share), BF16),
            pltpu.SemaphoreType.DMA((8,)),
            pltpu.SemaphoreType.DMA((PIECES,)),
            pltpu.SemaphoreType.DMA((5,)),
            pltpu.SemaphoreType.DMA((semaphores,)),
            pltpu.SemaphoreType.DMA((semaphores,)),
        ],
        compiler_params=pltpu.CompilerParams(
            collective_id=0, has_side_effects=True, vmem_limit_bytes=VMEM_LIMIT
        ),
        name="decoder",
    )(
        partners,
        counts,
        past_tokens.transpose(1, 0, 2),
        current.transpose(1, 0, 2),
        query_weight,
        key_weight,
        value_weight,
        output_weight,
        up_weight,
        down_weight,
    ).transpose(1, 0, 2)


def solution(mesh):
    placed = (
        P("pair", None, None),
        P("pair", None, None),
        P("pair"),
        P(),
        P(None, "mp"),
        P(None, "mp"),
        P(None, "mp"),
        P("mp", None),
        P(None, "mp"),
        P("mp", None),
    )
    return jax.shard_map(
        body, mesh=mesh, in_specs=placed, out_specs=P("pair", None, "mp"), check_vma=False
    )
```

```python
import functools
import math

import jax
import jax.numpy as jnp
from jax import lax
from jax.experimental import pallas as pl
from jax.experimental.pallas import tpu as pltpu
from jax.sharding import PartitionSpec as P

HEAD_DIM = 64
TILE = 16
LANES = 128
BLOCK_ROWS = 7
CUTS = (96, 240)
VMEM_LIMIT = 56 * 1024 * 1024
MESH = pl.DeviceIdType.MESH
F32 = jnp.float32
BF16 = jnp.bfloat16


class Ring:
    def __init__(self, part, rank, after, before, send, recv, base):
        def copy(index, owner, half, peer):
            ref = part(owner, half)
            return pltpu.make_async_remote_copy(
                src_ref=ref,
                dst_ref=ref,
                send_sem=send.at[base + index],
                recv_sem=recv.at[base + index],
                device_id={"mp": peer},
                device_id_type=MESH,
            )

        self.up = (copy(0, rank, 0, after), copy(1, rank, 1, after), copy(2, before, 0, after))
        self.down = (copy(3, rank, 1, before), copy(4, rank, 0, before), copy(5, after, 1, before))

    def start(self, step):
        self.up[step].start()
        self.down[step].start()

    def forward(self):
        self.up[0].wait_recv()
        self.up[2].start()
        self.down[0].wait_recv()
        self.down[2].start()

    def arrive(self):
        for step in (1, 2):
            self.up[step].wait_recv()
            self.down[step].wait_recv()

    def settle(self):
        for copy in self.up + self.down:
            copy.wait_send()


def normalized(values):
    center = values - jnp.mean(values, axis=-1, keepdims=True)
    spread = jnp.mean(center * center, axis=-1, keepdims=True)
    return (center * lax.rsqrt(spread + 1e-06)).astype(BF16)


def normalize(source, target, first, last):
    for start in range(first, last, TILE):
        stop = min(start + TILE, last)
        target[start:stop, :] = normalized(source[start:stop, :].astype(F32))


def flatten_and_normalize(source, target, first, last, kept=None):
    slots, width = source.shape[1:]
    for start in range(first, last, TILE):
        stop = min(start + TILE, last)
        tile = source[start // slots : stop // slots].reshape(stop - start, width)
        if kept is not None:
            kept[start:stop, :] = tile
        target[start:stop, :] = normalized(tile.astype(F32))


def put(target, first, last, result):
    for piece in range(target.shape[0]):
        target[piece, first:last, :] = result[:, piece * LANES : (piece + 1) * LANES]


def take(source, at):
    return jnp.concatenate([source[piece, at, :] for piece in range(source.shape[0])], axis=1)


def gelu(values):
    return 0.5 * values * (1.0 + lax.erf(values * (0.5**0.5)))


def decoder_kernel(
    groups,
    shards,
    partners_ref,
    counts_ref,
    past_hbm,
    current_hbm,
    query_hbm,
    key_hbm,
    value_hbm,
    output_hbm,
    up_hbm,
    down_hbm,
    out_ref,
    past,
    current,
    query_weight,
    key_weight,
    value_weight,
    output_weight,
    up_weight,
    down_weight,
    spread,
    sorted_tiles,
    context,
    flat,
    normed,
    queries,
    keys,
    values,
    mixed,
    attended,
    hidden,
    partial,
    packed,
    summed,
    landed,
    out,
    load,
    store,
    exchange_sem,
    ring_send,
    ring_recv,
):
    frame, slots, width = past.shape
    rows = frame * slots
    share = width // shards
    block_rows = spread.shape[1]
    halves = share // LANES
    kinds = frame // block_rows * halves
    side = math.isqrt(groups)
    keepers = kinds // side
    pieces = list(zip((0,) + CUTS, CUTS + (rows,)))
    last_piece = len(pieces) - 1
    me = lax.axis_index("pair")
    rank = lax.axis_index("mp")
    column = pl.multiple_of(rank * share, LANES)
    after = lax.rem(rank + 1, shards)
    before = lax.rem(rank + shards - 1, shards)
    across = lax.rem(rank + 2, shards)
    core = lax.rem(me, 2)
    twin = me + 1 - 2 * core

    def fetch(index, source, target):
        copy = pltpu.make_async_copy(source, target, load.at[index])
        copy.start()
        return copy

    get_past = fetch(0, past_hbm, past)
    get_output = fetch(
        1, output_hbm, output_weight.at[pl.ds(pl.multiple_of(rank * share, share), share), :]
    )
    get_current = fetch(2, current_hbm, current)
    get_query = fetch(3, query_hbm, query_weight)
    get_key = fetch(4, key_hbm, key_weight)
    get_value = fetch(5, value_hbm, value_weight)
    get_up = fetch(6, up_hbm, up_weight)
    get_down = fetch(7, down_hbm, down_weight)

    square = me // side
    seat = lax.rem(me, side)
    keeps = seat < keepers

    def place(kind):
        lane = pl.multiple_of(column + lax.rem(kind, halves) * LANES, LANES)
        return pl.ds(kind // halves * block_rows, block_rows), slice(None), pl.ds(lane, LANES)

    def other_square(step):
        offset = (step + 1) // 2 * (1 - 2 * lax.rem(step, 2))
        return lax.rem(square + side // 2 + offset, side)

    group = side // 2
    part = square // group
    corner = lax.rem(square, group)
    frame_part = frame // 2

    def delivery_squares():
        near = [part * group + lax.rem(corner + step, group) for step in (2, 1, 3)]
        far = [(1 - part) * group + lax.rem(corner + step, group) for step in (0, 1, 3, 2)]
        own = [square * side + lax.rem(seat + other, side) for other in range(1, side)]
        whole = [[there * side + other for other in range(side)] for there in near + far]
        return whole[:3] + [own] + whole[3:]

    def everyone(send):
        def one_square(step, carry):
            there = other_square(step)
            for other in range(side):
                send(there * side + other)
            return carry

        lax.fori_loop(0, side - 1, one_square, 0)
        for other in range(1, side):
            send(square * side + lax.rem(seat + other, side))

    barrier = pltpu.get_barrier_semaphore()

    def greet(peer):
        pl.semaphore_signal(barrier, inc=1, device_id={"pair": peer}, device_id_type=MESH)

    everyone(greet)
    for peer in (after, before):
        pl.semaphore_signal(barrier, inc=1, device_id={"mp": peer}, device_id_type=MESH)
    pl.semaphore_wait(barrier, groups + 1)

    get_past.wait()

    def spread_one(there, other):
        pltpu.make_async_remote_copy(
            src_ref=past.at[place(there * keepers + other)],
            dst_ref=spread.at[me],
            send_sem=exchange_sem.at[0],
            recv_sem=exchange_sem.at[1],
            device_id={"pair": there * side + other},
            device_id_type=MESH,
        ).start()

    def spread_square(step, carry):
        there = other_square(step)
        for other in range(keepers):
            spread_one(there, other)
        return carry

    lax.fori_loop(0, side - 1, spread_square, 0)
    mine = square * keepers + seat
    for other in range(keepers):
        pl.when(seat != other)(functools.partial(spread_one, square, other))

    @pl.when(keeps)
    def _():
        spread[me] = past[place(mine)]

    half = share // 2
    quarter = half // 2

    def weight_rows(owner, piece):
        row = pl.multiple_of(owner * share + core * half + piece * quarter, quarter)
        return output_weight.at[pl.ds(row, quarter), :]

    weight_ring = Ring(weight_rows, rank, after, before, ring_send, ring_recv, 0)
    get_output.wait()
    weight_ring.start(0)
    weight_ring.start(1)

    get_current.wait()
    get_query.wait()
    flatten_and_normalize(current, normed, 0, rows, flat)
    put(
        queries, 0, rows, jnp.dot(normed[0:rows, :], query_weight[...], preferred_element_type=F32)
    )

    weight_ring.forward()

    @pl.when(keeps)
    def _():
        arrived = spread.at[pl.ds(0, groups - 1)]
        pltpu.make_async_copy(arrived, arrived, exchange_sem.at[1]).wait()
        slot = lax.broadcasted_iota(jnp.int32, spread.shape[1:], 1)

        def sort_one(step):
            tile = spread[partners_ref[step * slots] // slots]
            for other in range(1, slots):
                tile = jnp.where(
                    slot == other, spread[partners_ref[step * slots + other] // slots], tile
                )
            sorted_tiles[step] = tile

        def deliver(target):
            pltpu.make_async_remote_copy(
                src_ref=sorted_tiles.at[target],
                dst_ref=context.at[place(mine)],
                send_sem=exchange_sem.at[2],
                recv_sem=exchange_sem.at[3 + part],
                device_id={"pair": target},
                device_id_type=MESH,
            ).start()

        waiting = []
        for targets in delivery_squares():
            for target in targets:
                sort_one(target)
            for target in waiting:
                deliver(target)
            waiting = targets
        sort_one(me)
        context[place(mine)] = sorted_tiles[me]
        for target in waiting:
            deliver(target)

    @pl.when(keeps)
    def _():
        got = spread.at[pl.ds(0, kinds // 2 - 1)]
        pltpu.make_async_copy(got, got, exchange_sem.at[3 + part]).wait()

    @pl.when(jnp.logical_not(keeps))
    def _():
        got = spread.at[pl.ds(0, kinds // 2)]
        pltpu.make_async_copy(got, got, exchange_sem.at[3 + part]).wait()

    def lanes_of(owner, piece):
        return pl.ds(pl.multiple_of(owner * share + piece * LANES, LANES), LANES)

    def context_part(index):
        size = frame_part // 2
        start = (part if index < 2 else 1 - part) * frame_part + index % 2 * size

        def of(owner, piece):
            return context.at[pl.ds(start, size), :, lanes_of(owner, piece)]

        return of

    def attended_part(first, last):
        def part(owner, piece):
            return attended.at[first:last, lanes_of(owner, piece)]

        return part

    def make_ring(of, base):
        return Ring(of, rank, after, before, ring_send, ring_recv, base)

    context_rings = [make_ring(context_part(k), 9 + 6 * k) for k in range(4)]
    attended_rings = [
        make_ring(attended_part(*piece), 33 + 6 * k) for k, piece in enumerate(pieces)
    ]

    def launch(ring):
        ring.start(0)
        ring.start(1)

    for ring in context_rings[:2]:
        ring.start(0)
    for ring in context_rings[:2]:
        ring.start(1)
    weight_ring.arrive()

    def to_twin(index, owner):
        row = pl.multiple_of(owner * share + core * half, half)
        ref = output_weight.at[pl.ds(row, half), :]
        return pltpu.make_async_remote_copy(
            src_ref=ref,
            dst_ref=ref,
            send_sem=ring_send.at[6 + index],
            recv_sem=ring_recv.at[6 + index],
            device_id={"pair": twin},
            device_id_type=MESH,
        )

    twins = [to_twin(index, owner) for index, owner in enumerate((before, after, across))]
    for copy in twins:
        copy.start()
    for ring in context_rings[:2]:
        ring.forward()
    got = spread.at[pl.ds(0, kinds // 2)]
    pltpu.make_async_copy(got, got, exchange_sem.at[3 + 1 - part]).wait()
    for ring in context_rings[2:]:
        ring.start(0)
    for ring in context_rings[2:]:
        ring.start(1)

    get_key.wait()
    get_value.wait()
    part_rows = frame_part * slots

    def project(index):
        at = part if index == 0 else 1 - part
        base = index * (normed.shape[0] // 2)
        for start in range(0, part_rows, TILE):
            count = min(TILE, part_rows - start)
            tile = context[pl.ds(at * frame_part + start // slots, count // slots)]
            normed[base + start : base + start + count, :] = normalized(
                tile.reshape(count, width).astype(F32)
            )
        for weight, target in ((key_weight, keys), (value_weight, values)):
            result = jnp.dot(
                normed[base : base + part_rows, :], weight[...], preferred_element_type=F32
            )
            for piece in range(halves):
                target[at, piece, 0:part_rows, :] = result[:, piece * LANES : (piece + 1) * LANES]

    for ring in context_rings[2:]:
        ring.forward()
    for index in range(2):
        for ring in context_rings[2 * index : 2 * index + 2]:
            ring.arrive()
        project(index)

    heads = share // HEAD_DIM

    def of_slot(source, slot):
        at = pl.ds(slot, frame_part, stride=slots)
        return jnp.concatenate([take(source.at[k], at) for k in range(2)], axis=0).astype(BF16)

    frame_keys = [of_slot(keys, slot) for slot in range(slots)]
    frame_values = [of_slot(values, slot) for slot in range(slots)]

    def attend(start, stop):
        count = -(-(stop - start) // slots // 8) * 8
        head_of = lax.broadcasted_iota(jnp.int32, (count, share), 1) // HEAD_DIM
        for slot in range(slots):
            at = pl.ds(start + slot, count, stride=slots)
            query = take(queries, at)
            stacked = jnp.concatenate(
                [jnp.where(head_of == head, query, 0.0) for head in range(heads)], axis=0
            ).astype(BF16)
            scores = (
                lax.dot_general(
                    stacked,
                    frame_keys[slot],
                    (((1,), (1,)), ((), ())),
                    preferred_element_type=F32,
                )
                * HEAD_DIM ** (-0.5)
            )
            lifted = jnp.exp(scores - jnp.max(scores, axis=-1, keepdims=True))
            weights = (lifted * (1.0 / jnp.sum(lifted, axis=-1, keepdims=True))).astype(BF16)
            spans = jnp.dot(weights, frame_values[slot], preferred_element_type=F32)
            total = spans[:count]
            for head in range(1, heads):
                total = jnp.where(head_of == head, spans[head * count : (head + 1) * count], total)
            for piece in range(mixed.shape[0]):
                mixed[piece, at, :] = total[:, piece * LANES : (piece + 1) * LANES]
        attended[start:stop, pl.ds(column, share)] = take(mixed, pl.ds(start, stop - start)).astype(
            BF16
        )

    for index, piece in enumerate(pieces):
        attend(*piece)
        if index < 2:
            launch(attended_rings[index])

    def sends(index, first, last):
        base = 33 + 6 * len(pieces) + 6 * index

        def copy(offset, source, peer):
            return pltpu.make_async_remote_copy(
                src_ref=source,
                dst_ref=landed.at[offset, first:last, :],
                send_sem=ring_send.at[base + offset],
                recv_sem=ring_recv.at[base + offset],
                device_id={"mp": peer},
                device_id_type=MESH,
            )

        return [
            copy(0, packed.at[first:last, lanes_of(across, 0)], after),
            copy(1, packed.at[first:last, lanes_of(across, 1)], before),
            copy(2, packed.at[first:last, lanes_of(after, 1)], after),
            copy(3, packed.at[first:last, lanes_of(before, 0)], before),
            copy(4, summed.at[0, first:last, :], after),
            copy(5, summed.at[1, first:last, :], before),
        ]

    reductions = [sends(index, *piece) for index, piece in enumerate(pieces)]

    def mix(index):
        first, last = pieces[index]
        hidden[first:last, :] = flat[first:last, :].astype(F32) + jnp.dot(
            attended[first:last, :], output_weight[...], preferred_element_type=F32
        )
        normalize(hidden, normed, first, last)
        expanded = gelu(
            jnp.dot(normed[first:last, :], up_weight[...], preferred_element_type=F32)
        ).astype(BF16)
        result = jnp.dot(expanded, down_weight[...], preferred_element_type=F32)
        partial[first:last, :] = result
        packed[first:last, :] = result.astype(BF16)
        for copy in reductions[index][:4]:
            copy.start()

    def relay(index):
        first, last = pieces[index]
        for piece, owner in ((0, after), (1, before)):
            reductions[index][piece].wait_recv()
            summed[piece, first:last, :] = (
                partial[first:last, lanes_of(owner, piece)]
                + landed[piece, first:last, :].astype(F32)
            ).astype(BF16)
            reductions[index][4 + piece].start()

    def finish(index):
        first, last = pieces[index]
        for copy in reductions[index][2:]:
            copy.wait_recv()
        for piece, others in ((0, (4, 3)), (1, (2, 5))):
            result = partial[first:last, lanes_of(rank, piece)]
            for other in others:
                result = result + landed[other, first:last, :].astype(F32)
            row = first + lax.broadcasted_iota(jnp.int32, result.shape, 0)
            limit = counts_ref[0]
            for slot in range(1, slots):
                limit = jnp.where(lax.rem(row, slots) == slot, counts_ref[slot], limit)
            result = hidden[first:last, lanes_of(rank, piece)] + result
            result = jnp.where(row // slots < limit, result, 0.0).astype(BF16)
            out[
                first // slots : last // slots, :, piece * LANES : (piece + 1) * LANES
            ] = result.reshape((last - first) // slots, slots, LANES)
        at = slice(first // slots, last // slots)
        pltpu.make_async_copy(out.at[at], out_ref.at[at], store.at[index]).start()

    for index in range(last_piece):
        attended_rings[index].forward()
        if index + 2 <= last_piece:
            launch(attended_rings[index + 2])
    for copy in twins:
        copy.wait_recv()
    get_up.wait()
    get_down.wait()
    for index, ring in enumerate(attended_rings):
        ring.arrive()
        mix(index)
        if index == 0:
            attended_rings[last_piece].forward()
        else:
            relay(index - 1)
    for index in range(last_piece - 1):
        finish(index)
    relay(last_piece)
    for index in range(last_piece - 1, last_piece + 1):
        finish(index)

    for index, (first, last) in enumerate(pieces):
        at = slice(first // slots, last // slots)
        pltpu.make_async_copy(out.at[at], out_ref.at[at], store.at[index]).wait()
    for ring in [weight_ring] + context_rings + attended_rings:
        ring.settle()
    for copy in twins + sum(reductions, []):
        copy.wait_send()

    @pl.when(keeps)
    def _():
        left = spread.at[pl.ds(0, kinds - 1)]
        pltpu.make_async_copy(left, left, exchange_sem.at[0]).wait()
        sent = spread.at[pl.ds(0, groups - 1)]
        pltpu.make_async_copy(sent, sent, exchange_sem.at[2]).wait()

    @pl.when(jnp.logical_not(keeps))
    def _():
        left = spread.at[pl.ds(0, kinds)]
        pltpu.make_async_copy(left, left, exchange_sem.at[0]).wait()


def body(
    current,
    past_tokens,
    counts,
    partners,
    query_weight,
    key_weight,
    value_weight,
    output_weight,
    up_weight,
    down_weight,
):
    slots, frame, width = current.shape
    groups, shards = lax.axis_size("pair"), lax.axis_size("mp")
    share = width // shards
    features = query_weight.shape[1]
    hidden_units = up_weight.shape[1]
    rows = slots * frame
    spare = rows + TILE
    half_rows = -(-rows // 2 // TILE) * TILE
    whole = pl.BlockSpec(memory_space=pltpu.HBM)
    packed_shape = (frame, slots, width)
    semaphores = 33 + 12 * (len(CUTS) + 1)
    return pl.pallas_call(
        functools.partial(decoder_kernel, groups, shards),
        out_shape=jax.ShapeDtypeStruct((frame, slots, share), BF16),
        in_specs=[pl.BlockSpec(memory_space=pltpu.SMEM)] * 2 + [whole] * 8,
        out_specs=whole,
        scratch_shapes=[
            pltpu.VMEM(packed_shape, BF16),
            pltpu.VMEM(packed_shape, BF16),
            pltpu.VMEM((width, features), BF16),
            pltpu.VMEM((width, features), BF16),
            pltpu.VMEM((width, features), BF16),
            pltpu.VMEM((width, width), BF16),
            pltpu.VMEM((width, hidden_units), BF16),
            pltpu.VMEM((hidden_units, width), BF16),
            pltpu.VMEM((groups, BLOCK_ROWS, slots, LANES), BF16),
            pltpu.VMEM((groups, BLOCK_ROWS, slots, LANES), BF16),
            pltpu.VMEM(packed_shape, BF16),
            pltpu.VMEM((rows, width), BF16),
            pltpu.VMEM((2 * half_rows, width), BF16),
            pltpu.VMEM((features // LANES, spare, LANES), F32),
            pltpu.VMEM((2, features // LANES, half_rows, LANES), F32),
            pltpu.VMEM((2, features // LANES, half_rows, LANES), F32),
            pltpu.VMEM((features // LANES, spare, LANES), F32),
            pltpu.VMEM((rows, width), BF16),
            pltpu.VMEM((rows, width), F32),
            pltpu.VMEM((rows, width), F32),
            pltpu.VMEM((rows, width), BF16),
            pltpu.VMEM((2, rows, LANES), BF16),
            pltpu.VMEM((6, rows, LANES), BF16),
            pltpu.VMEM((frame, slots, share), BF16),
            pltpu.SemaphoreType.DMA((8,)),
            pltpu.SemaphoreType.DMA((len(CUTS) + 1,)),
            pltpu.SemaphoreType.DMA((5,)),
            pltpu.SemaphoreType.DMA((semaphores,)),
            pltpu.SemaphoreType.DMA((semaphores,)),
        ],
        compiler_params=pltpu.CompilerParams(
            collective_id=0, has_side_effects=True, vmem_limit_bytes=VMEM_LIMIT
        ),
        name="decoder",
    )(
        partners,
        counts,
        past_tokens.transpose(1, 0, 2),
        current.transpose(1, 0, 2),
        query_weight,
        key_weight,
        value_weight,
        output_weight,
        up_weight,
        down_weight,
    ).transpose(1, 0, 2)


def solution(mesh):
    placed = (
        P("pair", None, None),
        P("pair", None, None),
        P("pair"),
        P(),
        P(None, "mp"),
        P(None, "mp"),
        P(None, "mp"),
        P("mp", None),
        P(None, "mp"),
        P("mp", None),
    )
    return jax.shard_map(
        body, mesh=mesh, in_specs=placed, out_specs=P("pair", None, "mp"), check_vma=False
    )
```

```python
import functools
import math

import jax
import jax.numpy as jnp
from jax import lax
from jax.experimental import pallas as pl
from jax.experimental.pallas import tpu as pltpu
from jax.sharding import PartitionSpec as P

HEAD_DIM = 64
TILE = 16
LANES = 128
BLOCK_ROWS = 7
CUTS = (112, 272)
VMEM_LIMIT = 54784 * 1024
MESH = pl.DeviceIdType.MESH
F32 = jnp.float32
BF16 = jnp.bfloat16


class Ring:
    def __init__(self, part, rank, after, before, send, recv, base):
        def copy(index, owner, half, peer):
            ref = part(owner, half)
            return pltpu.make_async_remote_copy(
                src_ref=ref,
                dst_ref=ref,
                send_sem=send.at[base + index],
                recv_sem=recv.at[base + index],
                device_id={"mp": peer},
                device_id_type=MESH,
            )

        self.up = (copy(0, rank, 0, after), copy(1, rank, 1, after), copy(2, before, 0, after))
        self.down = (copy(3, rank, 1, before), copy(4, rank, 0, before), copy(5, after, 1, before))

    def start(self, step):
        self.up[step].start()
        self.down[step].start()

    def forward(self):
        self.up[0].wait_recv()
        self.up[2].start()
        self.down[0].wait_recv()
        self.down[2].start()

    def arrive(self):
        for step in (1, 2):
            self.up[step].wait_recv()
            self.down[step].wait_recv()

    def settle(self):
        for copy in self.up + self.down:
            copy.wait_send()


def normalized(values):
    center = values - jnp.mean(values, axis=-1, keepdims=True)
    spread = jnp.mean(center * center, axis=-1, keepdims=True)
    return (center * lax.rsqrt(spread + 1e-06)).astype(BF16)


def normalize(source, target, first, last):
    for start in range(first, last, TILE):
        stop = min(start + TILE, last)
        target[start:stop, :] = normalized(source[start:stop, :].astype(F32))


def flatten_and_normalize(source, target, first, last, kept=None):
    slots, width = source.shape[1:]
    for start in range(first, last, TILE):
        stop = min(start + TILE, last)
        tile = source[start // slots : stop // slots].reshape(stop - start, width)
        if kept is not None:
            kept[start:stop, :] = tile
        target[start:stop, :] = normalized(tile.astype(F32))


def put(target, first, last, result):
    for piece in range(target.shape[0]):
        target[piece, first:last, :] = result[:, piece * LANES : (piece + 1) * LANES]


def take(source, at):
    return jnp.concatenate([source[piece, at, :] for piece in range(source.shape[0])], axis=1)


def gelu(values):
    return 0.5 * values * (1.0 + lax.erf(values * (0.5**0.5)))


def decoder_kernel(
    groups,
    shards,
    partners_ref,
    counts_ref,
    past_hbm,
    current_hbm,
    query_hbm,
    key_hbm,
    value_hbm,
    output_hbm,
    up_hbm,
    down_hbm,
    out_ref,
    past,
    current,
    query_weight,
    key_weight,
    value_weight,
    output_weight,
    up_weight,
    down_weight,
    spread,
    sorted_tiles,
    context,
    flat,
    normed,
    queries,
    keys,
    values,
    mixed,
    attended,
    hidden,
    partial,
    packed,
    summed,
    landed,
    load,
    exchange_sem,
    ring_send,
    ring_recv,
):
    frame, slots, width = past.shape
    rows = frame * slots
    share = width // shards
    block_rows = spread.shape[1]
    halves = share // LANES
    kinds = frame // block_rows * halves
    side = math.isqrt(groups)
    keepers = kinds // side
    pieces = list(zip((0,) + CUTS, CUTS + (rows,)))
    last_piece = len(pieces) - 1
    me = lax.axis_index("pair")
    rank = lax.axis_index("mp")
    column = pl.multiple_of(rank * share, LANES)
    after = lax.rem(rank + 1, shards)
    before = lax.rem(rank + shards - 1, shards)
    across = lax.rem(rank + 2, shards)
    core = lax.rem(me, 2)
    twin = me + 1 - 2 * core

    def fetch(index, source, target):
        copy = pltpu.make_async_copy(source, target, load.at[index])
        copy.start()
        return copy

    get_past = fetch(0, past_hbm, past)
    get_output = fetch(
        1, output_hbm, output_weight.at[pl.ds(pl.multiple_of(rank * share, share), share), :]
    )
    get_current = fetch(2, current_hbm, current)
    get_query = fetch(3, query_hbm, query_weight)
    get_key = fetch(4, key_hbm, key_weight)
    get_value = fetch(5, value_hbm, value_weight)
    get_up = fetch(6, up_hbm, up_weight)
    get_down = fetch(7, down_hbm, down_weight)

    square = me // side
    seat = lax.rem(me, side)
    keeps = seat < keepers

    def place(kind):
        lane = pl.multiple_of(column + lax.rem(kind, halves) * LANES, LANES)
        return pl.ds(kind // halves * block_rows, block_rows), slice(None), pl.ds(lane, LANES)

    def other_square(step):
        offset = (step + 1) // 2 * (1 - 2 * lax.rem(step, 2))
        return lax.rem(square + side // 2 + offset, side)

    group = side // 2
    part = square // group
    corner = lax.rem(square, group)
    frame_part = frame // 2

    def delivery_squares():
        near = [part * group + lax.rem(corner + step, group) for step in (2, 1, 3)]
        far = [(1 - part) * group + lax.rem(corner + step, group) for step in (0, 1, 3, 2)]
        own = [square * side + lax.rem(seat + other, side) for other in range(1, side)]
        whole = [[there * side + other for other in range(side)] for there in near + far]
        return whole[:3] + [own] + whole[3:]

    def everyone(send):
        def one_square(step, carry):
            there = other_square(step)
            for other in range(side):
                send(there * side + other)
            return carry

        lax.fori_loop(0, side - 1, one_square, 0)
        for other in range(1, side):
            send(square * side + lax.rem(seat + other, side))

    barrier = pltpu.get_barrier_semaphore()

    def greet(peer):
        pl.semaphore_signal(barrier, inc=1, device_id={"pair": peer}, device_id_type=MESH)

    everyone(greet)
    for peer in (after, before):
        pl.semaphore_signal(barrier, inc=1, device_id={"mp": peer}, device_id_type=MESH)
    pl.semaphore_wait(barrier, groups + 1)

    get_past.wait()

    def spread_one(there, other):
        pltpu.make_async_remote_copy(
            src_ref=past.at[place(there * keepers + other)],
            dst_ref=spread.at[me],
            send_sem=exchange_sem.at[0],
            recv_sem=exchange_sem.at[1],
            device_id={"pair": there * side + other},
            device_id_type=MESH,
        ).start()

    def spread_square(step, carry):
        there = other_square(step)
        for other in range(keepers):
            spread_one(there, other)
        return carry

    lax.fori_loop(0, side - 1, spread_square, 0)
    mine = square * keepers + seat
    for other in range(keepers):
        pl.when(seat != other)(functools.partial(spread_one, square, other))

    @pl.when(keeps)
    def _():
        spread[me] = past[place(mine)]

    half = share // 2
    quarter = half // 2

    def weight_rows(owner, piece):
        row = pl.multiple_of(owner * share + core * half + piece * quarter, quarter)
        return output_weight.at[pl.ds(row, quarter), :]

    weight_ring = Ring(weight_rows, rank, after, before, ring_send, ring_recv, 0)
    get_output.wait()
    weight_ring.start(0)
    weight_ring.start(1)

    get_current.wait()
    get_query.wait()
    flatten_and_normalize(current, normed, 0, rows, flat)
    put(
        queries, 0, rows, jnp.dot(normed[0:rows, :], query_weight[...], preferred_element_type=F32)
    )

    weight_ring.forward()

    @pl.when(keeps)
    def _():
        arrived = spread.at[pl.ds(0, groups - 1)]
        pltpu.make_async_copy(arrived, arrived, exchange_sem.at[1]).wait()
        slot = lax.broadcasted_iota(jnp.int32, spread.shape[1:], 1)

        def sort_one(step):
            tile = spread[partners_ref[step * slots] // slots]
            for other in range(1, slots):
                tile = jnp.where(
                    slot == other, spread[partners_ref[step * slots + other] // slots], tile
                )
            sorted_tiles[step] = tile

        def deliver(target):
            pltpu.make_async_remote_copy(
                src_ref=sorted_tiles.at[target],
                dst_ref=context.at[place(mine)],
                send_sem=exchange_sem.at[2],
                recv_sem=exchange_sem.at[3 + part],
                device_id={"pair": target},
                device_id_type=MESH,
            ).start()

        waiting = []
        for targets in delivery_squares():
            for target in targets:
                sort_one(target)
            for target in waiting:
                deliver(target)
            waiting = targets
        sort_one(me)
        context[place(mine)] = sorted_tiles[me]
        for target in waiting:
            deliver(target)

    @pl.when(keeps)
    def _():
        got = spread.at[pl.ds(0, kinds // 2 - 1)]
        pltpu.make_async_copy(got, got, exchange_sem.at[3 + part]).wait()

    @pl.when(jnp.logical_not(keeps))
    def _():
        got = spread.at[pl.ds(0, kinds // 2)]
        pltpu.make_async_copy(got, got, exchange_sem.at[3 + part]).wait()

    def lanes_of(owner, piece):
        return pl.ds(pl.multiple_of(owner * share + piece * LANES, LANES), LANES)

    def context_part(index):
        size = frame_part // 2
        start = (part if index < 2 else 1 - part) * frame_part + index % 2 * size

        def of(owner, piece):
            return context.at[pl.ds(start, size), :, lanes_of(owner, piece)]

        return of

    def attended_part(first, last):
        def part(owner, piece):
            return attended.at[first:last, lanes_of(owner, piece)]

        return part

    def make_ring(of, base):
        return Ring(of, rank, after, before, ring_send, ring_recv, base)

    context_rings = [make_ring(context_part(k), 9 + 6 * k) for k in range(4)]
    attended_rings = [
        make_ring(attended_part(*piece), 33 + 6 * k) for k, piece in enumerate(pieces)
    ]

    def launch(ring):
        ring.start(0)
        ring.start(1)

    for ring in context_rings[:2]:
        ring.start(0)
    for ring in context_rings[:2]:
        ring.start(1)
    weight_ring.arrive()

    def to_twin(index, owner):
        row = pl.multiple_of(owner * share + core * half, half)
        ref = output_weight.at[pl.ds(row, half), :]
        return pltpu.make_async_remote_copy(
            src_ref=ref,
            dst_ref=ref,
            send_sem=ring_send.at[6 + index],
            recv_sem=ring_recv.at[6 + index],
            device_id={"pair": twin},
            device_id_type=MESH,
        )

    twins = [to_twin(index, owner) for index, owner in enumerate((before, after, across))]
    for copy in twins:
        copy.start()
    for ring in context_rings[:2]:
        ring.forward()
    got = spread.at[pl.ds(0, kinds // 2)]
    pltpu.make_async_copy(got, got, exchange_sem.at[3 + 1 - part]).wait()
    for ring in context_rings[2:]:
        ring.start(0)
    for ring in context_rings[2:]:
        ring.start(1)

    get_key.wait()
    get_value.wait()
    part_rows = frame_part * slots

    def project(index):
        at = part if index == 0 else 1 - part
        base = index * (normed.shape[0] // 2)
        for start in range(0, part_rows, TILE):
            count = min(TILE, part_rows - start)
            tile = context[pl.ds(at * frame_part + start // slots, count // slots)]
            normed[base + start : base + start + count, :] = normalized(
                tile.reshape(count, width).astype(F32)
            )
        for weight, target in ((key_weight, keys), (value_weight, values)):
            result = jnp.dot(
                normed[base : base + part_rows, :], weight[...], preferred_element_type=F32
            )
            for piece in range(halves):
                target[at, piece, 0:part_rows, :] = result[:, piece * LANES : (piece + 1) * LANES]

    for ring in context_rings[2:]:
        ring.forward()
    for index in range(2):
        for ring in context_rings[2 * index : 2 * index + 2]:
            ring.arrive()
        project(index)

    heads = share // HEAD_DIM

    def of_slot(source, slot):
        at = pl.ds(slot, frame_part, stride=slots)
        return jnp.concatenate([take(source.at[k], at) for k in range(2)], axis=0).astype(BF16)

    frame_keys = [of_slot(keys, slot) for slot in range(slots)]
    frame_values = [of_slot(values, slot) for slot in range(slots)]

    def attend(start, stop):
        count = -(-(stop - start) // slots // 8) * 8
        head_of = lax.broadcasted_iota(jnp.int32, (count, share), 1) // HEAD_DIM
        for slot in range(slots):
            at = pl.ds(start + slot, count, stride=slots)
            query = take(queries, at)
            stacked = jnp.concatenate(
                [jnp.where(head_of == head, query, 0.0) for head in range(heads)], axis=0
            ).astype(BF16)
            scores = (
                lax.dot_general(
                    stacked,
                    frame_keys[slot],
                    (((1,), (1,)), ((), ())),
                    preferred_element_type=F32,
                )
                * HEAD_DIM ** (-0.5)
            )
            lifted = jnp.exp(scores - jnp.max(scores, axis=-1, keepdims=True))
            weights = (lifted * (1.0 / jnp.sum(lifted, axis=-1, keepdims=True))).astype(BF16)
            spans = jnp.dot(weights, frame_values[slot], preferred_element_type=F32)
            total = spans[:count]
            for head in range(1, heads):
                total = jnp.where(head_of == head, spans[head * count : (head + 1) * count], total)
            for piece in range(mixed.shape[0]):
                mixed[piece, at, :] = total[:, piece * LANES : (piece + 1) * LANES]
        attended[start:stop, pl.ds(column, share)] = take(mixed, pl.ds(start, stop - start)).astype(
            BF16
        )

    for index, piece in enumerate(pieces):
        attend(*piece)
        if index < 2:
            launch(attended_rings[index])

    def sends(index, first, last):
        base = 33 + 6 * len(pieces) + 6 * index

        def copy(offset, source, peer):
            return pltpu.make_async_remote_copy(
                src_ref=source,
                dst_ref=landed.at[offset, first:last, :],
                send_sem=ring_send.at[base + offset],
                recv_sem=ring_recv.at[base + offset],
                device_id={"mp": peer},
                device_id_type=MESH,
            )

        return [
            copy(0, packed.at[first:last, lanes_of(across, 0)], after),
            copy(1, packed.at[first:last, lanes_of(across, 1)], before),
            copy(2, packed.at[first:last, lanes_of(after, 1)], after),
            copy(3, packed.at[first:last, lanes_of(before, 0)], before),
            copy(4, summed.at[0, first:last, :], after),
            copy(5, summed.at[1, first:last, :], before),
        ]

    reductions = [sends(index, *piece) for index, piece in enumerate(pieces)]

    def mix(index):
        first, last = pieces[index]
        hidden[first:last, :] = flat[first:last, :].astype(F32) + jnp.dot(
            attended[first:last, :], output_weight[...], preferred_element_type=F32
        )
        normalize(hidden, normed, first, last)
        expanded = gelu(
            jnp.dot(normed[first:last, :], up_weight[...], preferred_element_type=F32)
        ).astype(BF16)
        result = jnp.dot(expanded, down_weight[...], preferred_element_type=F32)
        partial[first:last, :] = result
        packed[first:last, :] = result.astype(BF16)
        for copy in reductions[index][:4]:
            copy.start()

    def relay(index):
        first, last = pieces[index]
        for piece, owner in ((0, after), (1, before)):
            reductions[index][piece].wait_recv()
            summed[piece, first:last, :] = (
                partial[first:last, lanes_of(owner, piece)]
                + landed[piece, first:last, :].astype(F32)
            ).astype(BF16)
            reductions[index][4 + piece].start()

    def finish(index):
        first, last = pieces[index]
        for copy in reductions[index][2:]:
            copy.wait_recv()
        for piece, others in ((0, (4, 3)), (1, (2, 5))):
            result = partial[first:last, lanes_of(rank, piece)]
            for other in others:
                result = result + landed[other, first:last, :].astype(F32)
            row = first + lax.broadcasted_iota(jnp.int32, result.shape, 0)
            limit = counts_ref[0]
            for slot in range(1, slots):
                limit = jnp.where(lax.rem(row, slots) == slot, counts_ref[slot], limit)
            result = hidden[first:last, lanes_of(rank, piece)] + result
            result = jnp.where(row // slots < limit, result, 0.0).astype(BF16)
            out_ref[
                first // slots : last // slots, :, piece * LANES : (piece + 1) * LANES
            ] = result.reshape((last - first) // slots, slots, LANES)

    for index in range(last_piece):
        attended_rings[index].forward()
        if index + 2 <= last_piece:
            launch(attended_rings[index + 2])
    for copy in twins:
        copy.wait_recv()
    get_up.wait()
    get_down.wait()
    for index, ring in enumerate(attended_rings):
        ring.arrive()
        mix(index)
        if index == 0:
            attended_rings[last_piece].forward()
        else:
            relay(index - 1)
    for index in range(last_piece - 1):
        finish(index)
    relay(last_piece)
    for index in range(last_piece - 1, last_piece + 1):
        finish(index)

    for ring in [weight_ring] + context_rings + attended_rings:
        ring.settle()
    for copy in twins + sum(reductions, []):
        copy.wait_send()

    @pl.when(keeps)
    def _():
        left = spread.at[pl.ds(0, kinds - 1)]
        pltpu.make_async_copy(left, left, exchange_sem.at[0]).wait()
        sent = spread.at[pl.ds(0, groups - 1)]
        pltpu.make_async_copy(sent, sent, exchange_sem.at[2]).wait()

    @pl.when(jnp.logical_not(keeps))
    def _():
        left = spread.at[pl.ds(0, kinds)]
        pltpu.make_async_copy(left, left, exchange_sem.at[0]).wait()


def body(
    current,
    past_tokens,
    counts,
    partners,
    query_weight,
    key_weight,
    value_weight,
    output_weight,
    up_weight,
    down_weight,
):
    slots, frame, width = current.shape
    groups, shards = lax.axis_size("pair"), lax.axis_size("mp")
    share = width // shards
    features = query_weight.shape[1]
    hidden_units = up_weight.shape[1]
    rows = slots * frame
    spare = rows + TILE
    half_rows = -(-rows // 2 // TILE) * TILE
    whole = pl.BlockSpec(memory_space=pltpu.HBM)
    packed_shape = (frame, slots, width)
    semaphores = 33 + 12 * (len(CUTS) + 1)
    return pl.pallas_call(
        functools.partial(decoder_kernel, groups, shards),
        out_shape=jax.ShapeDtypeStruct((frame, slots, share), BF16),
        in_specs=[pl.BlockSpec(memory_space=pltpu.SMEM)] * 2 + [whole] * 8,
        out_specs=pl.BlockSpec(memory_space=pltpu.VMEM),
        scratch_shapes=[
            pltpu.VMEM(packed_shape, BF16),
            pltpu.VMEM(packed_shape, BF16),
            pltpu.VMEM((width, features), BF16),
            pltpu.VMEM((width, features), BF16),
            pltpu.VMEM((width, features), BF16),
            pltpu.VMEM((width, width), BF16),
            pltpu.VMEM((width, hidden_units), BF16),
            pltpu.VMEM((hidden_units, width), BF16),
            pltpu.VMEM((groups, BLOCK_ROWS, slots, LANES), BF16),
            pltpu.VMEM((groups, BLOCK_ROWS, slots, LANES), BF16),
            pltpu.VMEM(packed_shape, BF16),
            pltpu.VMEM((rows, width), BF16),
            pltpu.VMEM((2 * half_rows, width), BF16),
            pltpu.VMEM((features // LANES, spare, LANES), F32),
            pltpu.VMEM((2, features // LANES, half_rows, LANES), F32),
            pltpu.VMEM((2, features // LANES, half_rows, LANES), F32),
            pltpu.VMEM((features // LANES, spare, LANES), F32),
            pltpu.VMEM((rows, width), BF16),
            pltpu.VMEM((rows, width), F32),
            pltpu.VMEM((rows, width), F32),
            pltpu.VMEM((rows, width), BF16),
            pltpu.VMEM((2, rows, LANES), BF16),
            pltpu.VMEM((6, rows, LANES), BF16),
            pltpu.SemaphoreType.DMA((8,)),
            pltpu.SemaphoreType.DMA((5,)),
            pltpu.SemaphoreType.DMA((semaphores,)),
            pltpu.SemaphoreType.DMA((semaphores,)),
        ],
        compiler_params=pltpu.CompilerParams(
            collective_id=0, has_side_effects=True, vmem_limit_bytes=VMEM_LIMIT
        ),
        name="decoder",
    )(
        partners,
        counts,
        past_tokens.transpose(1, 0, 2),
        current.transpose(1, 0, 2),
        query_weight,
        key_weight,
        value_weight,
        output_weight,
        up_weight,
        down_weight,
    ).transpose(1, 0, 2)


def solution(mesh):
    placed = (
        P("pair", None, None),
        P("pair", None, None),
        P("pair"),
        P(),
        P(None, "mp"),
        P(None, "mp"),
        P(None, "mp"),
        P("mp", None),
        P(None, "mp"),
        P("mp", None),
    )
    return jax.shard_map(
        body, mesh=mesh, in_specs=placed, out_specs=P("pair", None, "mp"), check_vma=False
    )
```

```python
import functools
import math

import jax
import jax.numpy as jnp
from jax import lax
from jax.experimental import pallas as pl
from jax.experimental.pallas import tpu as pltpu
from jax.sharding import PartitionSpec as P

HEAD_DIM = 64
TILE = 16
LANES = 128
BLOCK_ROWS = 7
CUTS = (112, 272)
VMEM_LIMIT = 54784 * 1024
MESH = pl.DeviceIdType.MESH
F32 = jnp.float32
BF16 = jnp.bfloat16


class Ring:
    def __init__(self, part, rank, after, before, send, recv, base):
        def copy(index, owner, half, peer):
            ref = part(owner, half)
            return pltpu.make_async_remote_copy(
                src_ref=ref,
                dst_ref=ref,
                send_sem=send.at[base + index],
                recv_sem=recv.at[base + index],
                device_id={"mp": peer},
                device_id_type=MESH,
            )

        self.up = (copy(0, rank, 0, after), copy(1, rank, 1, after), copy(2, before, 0, after))
        self.down = (copy(3, rank, 1, before), copy(4, rank, 0, before), copy(5, after, 1, before))

    def start(self, step):
        self.up[step].start()
        self.down[step].start()

    def forward(self):
        self.up[0].wait_recv()
        self.up[2].start()
        self.down[0].wait_recv()
        self.down[2].start()

    def arrive(self):
        for step in (1, 2):
            self.up[step].wait_recv()
            self.down[step].wait_recv()

    def settle(self):
        for copy in self.up + self.down:
            copy.wait_send()


def normalized(values):
    center = values - jnp.mean(values, axis=-1, keepdims=True)
    spread = jnp.mean(center * center, axis=-1, keepdims=True)
    return (center * lax.rsqrt(spread + 1e-06)).astype(BF16)


def normalize(source, target, first, last):
    for start in range(first, last, TILE):
        stop = min(start + TILE, last)
        target[start:stop, :] = normalized(source[start:stop, :].astype(F32))


def flatten_and_normalize(source, target, first, last, kept=None):
    slots, width = source.shape[1:]
    for start in range(first, last, TILE):
        stop = min(start + TILE, last)
        tile = source[start // slots : stop // slots].reshape(stop - start, width)
        if kept is not None:
            kept[start:stop, :] = tile
        target[start:stop, :] = normalized(tile.astype(F32))


def put(target, first, last, result):
    for piece in range(target.shape[0]):
        target[piece, first:last, :] = result[:, piece * LANES : (piece + 1) * LANES]


def take(source, at):
    return jnp.concatenate([source[piece, at, :] for piece in range(source.shape[0])], axis=1)


def gelu(values):
    return 0.5 * values * (1.0 + lax.erf(values * (0.5**0.5)))


def decoder_kernel(
    groups,
    shards,
    table_ref,
    past_hbm,
    current_hbm,
    query_hbm,
    key_hbm,
    value_hbm,
    output_hbm,
    up_hbm,
    down_hbm,
    out_ref,
    past,
    current,
    query_weight,
    key_weight,
    value_weight,
    output_weight,
    up_weight,
    down_weight,
    spread,
    sorted_tiles,
    context,
    flat,
    normed,
    queries,
    keys,
    values,
    mixed,
    attended,
    hidden,
    partial,
    packed,
    summed,
    landed,
    load,
    exchange_sem,
    ring_send,
    ring_recv,
):
    frame, slots, width = past.shape
    rows = frame * slots
    share = width // shards
    block_rows = spread.shape[1]
    halves = share // LANES
    kinds = frame // block_rows * halves
    side = math.isqrt(groups)
    keepers = kinds // side
    pieces = list(zip((0,) + CUTS, CUTS + (rows,)))
    last_piece = len(pieces) - 1
    me = lax.axis_index("pair")
    rank = lax.axis_index("mp")
    column = pl.multiple_of(rank * share, LANES)
    after = lax.rem(rank + 1, shards)
    before = lax.rem(rank + shards - 1, shards)
    across = lax.rem(rank + 2, shards)
    core = lax.rem(me, 2)
    twin = me + 1 - 2 * core

    def fetch(index, source, target):
        copy = pltpu.make_async_copy(source, target, load.at[index])
        copy.start()
        return copy

    get_past = fetch(0, past_hbm, past)
    get_output = fetch(
        1, output_hbm, output_weight.at[pl.ds(pl.multiple_of(rank * share, share), share), :]
    )
    get_current = fetch(2, current_hbm, current)
    get_query = fetch(3, query_hbm, query_weight)
    get_key = fetch(4, key_hbm, key_weight)
    get_value = fetch(5, value_hbm, value_weight)
    get_up = fetch(6, up_hbm, up_weight)
    get_down = fetch(7, down_hbm, down_weight)

    square = me // side
    seat = lax.rem(me, side)
    keeps = seat < keepers

    def place(kind):
        lane = pl.multiple_of(column + lax.rem(kind, halves) * LANES, LANES)
        return pl.ds(kind // halves * block_rows, block_rows), slice(None), pl.ds(lane, LANES)

    def other_square(step):
        offset = (step + 1) // 2 * (1 - 2 * lax.rem(step, 2))
        return lax.rem(square + side // 2 + offset, side)

    group = side // 2
    part = square // group
    corner = lax.rem(square, group)
    frame_part = frame // 2

    def delivery_squares():
        near = [part * group + lax.rem(corner + step, group) for step in (2, 1, 3)]
        far = [(1 - part) * group + lax.rem(corner + step, group) for step in (0, 1, 3, 2)]
        own = [square * side + lax.rem(seat + other, side) for other in range(1, side)]
        whole = [[there * side + other for other in range(side)] for there in near + far]
        return whole[:3] + [own] + whole[3:]

    def everyone(send):
        def one_square(step, carry):
            there = other_square(step)
            for other in range(side):
                send(there * side + other)
            return carry

        lax.fori_loop(0, side - 1, one_square, 0)
        for other in range(1, side):
            send(square * side + lax.rem(seat + other, side))

    barrier = pltpu.get_barrier_semaphore()

    def greet(peer):
        pl.semaphore_signal(barrier, inc=1, device_id={"pair": peer}, device_id_type=MESH)

    everyone(greet)
    for peer in (after, before):
        pl.semaphore_signal(barrier, inc=1, device_id={"mp": peer}, device_id_type=MESH)
    pl.semaphore_wait(barrier, groups + 1)

    get_past.wait()

    def spread_one(there, other):
        pltpu.make_async_remote_copy(
            src_ref=past.at[place(there * keepers + other)],
            dst_ref=spread.at[me],
            send_sem=exchange_sem.at[0],
            recv_sem=exchange_sem.at[1],
            device_id={"pair": there * side + other},
            device_id_type=MESH,
        ).start()

    def spread_square(step, carry):
        there = other_square(step)
        for other in range(keepers):
            spread_one(there, other)
        return carry

    lax.fori_loop(0, side - 1, spread_square, 0)
    mine = square * keepers + seat
    for other in range(keepers):
        pl.when(seat != other)(functools.partial(spread_one, square, other))

    @pl.when(keeps)
    def _():
        spread[me] = past[place(mine)]

    half = share // 2
    quarter = half // 2

    def weight_rows(owner, piece):
        row = pl.multiple_of(owner * share + core * half + piece * quarter, quarter)
        return output_weight.at[pl.ds(row, quarter), :]

    weight_ring = Ring(weight_rows, rank, after, before, ring_send, ring_recv, 0)
    get_output.wait()
    weight_ring.start(0)
    weight_ring.start(1)

    get_current.wait()
    get_query.wait()
    flatten_and_normalize(current, normed, 0, rows, flat)
    put(
        queries, 0, rows, jnp.dot(normed[0:rows, :], query_weight[...], preferred_element_type=F32)
    )

    weight_ring.forward()

    @pl.when(keeps)
    def _():
        arrived = spread.at[pl.ds(0, groups - 1)]
        pltpu.make_async_copy(arrived, arrived, exchange_sem.at[1]).wait()
        slot = lax.broadcasted_iota(jnp.int32, spread.shape[1:], 1)

        def sort_one(step):
            tile = spread[table_ref[step * slots] // slots]
            for other in range(1, slots):
                tile = jnp.where(
                    slot == other, spread[table_ref[step * slots + other] // slots], tile
                )
            sorted_tiles[step] = tile

        def deliver(target):
            pltpu.make_async_remote_copy(
                src_ref=sorted_tiles.at[target],
                dst_ref=context.at[place(mine)],
                send_sem=exchange_sem.at[2],
                recv_sem=exchange_sem.at[3 + part],
                device_id={"pair": target},
                device_id_type=MESH,
            ).start()

        waiting = []
        for targets in delivery_squares():
            for target in targets:
                sort_one(target)
            for target in waiting:
                deliver(target)
            waiting = targets
        sort_one(me)
        context[place(mine)] = sorted_tiles[me]
        for target in waiting:
            deliver(target)

    @pl.when(keeps)
    def _():
        got = spread.at[pl.ds(0, kinds // 2 - 1)]
        pltpu.make_async_copy(got, got, exchange_sem.at[3 + part]).wait()

    @pl.when(jnp.logical_not(keeps))
    def _():
        got = spread.at[pl.ds(0, kinds // 2)]
        pltpu.make_async_copy(got, got, exchange_sem.at[3 + part]).wait()

    def lanes_of(owner, piece):
        return pl.ds(pl.multiple_of(owner * share + piece * LANES, LANES), LANES)

    def context_part(index):
        size = frame_part // 2
        start = (part if index < 2 else 1 - part) * frame_part + index % 2 * size

        def of(owner, piece):
            return context.at[pl.ds(start, size), :, lanes_of(owner, piece)]

        return of

    def attended_part(first, last):
        def part(owner, piece):
            return attended.at[first:last, lanes_of(owner, piece)]

        return part

    def make_ring(of, base):
        return Ring(of, rank, after, before, ring_send, ring_recv, base)

    context_rings = [make_ring(context_part(k), 9 + 6 * k) for k in range(4)]
    attended_rings = [
        make_ring(attended_part(*piece), 33 + 6 * k) for k, piece in enumerate(pieces)
    ]

    def launch(ring):
        ring.start(0)
        ring.start(1)

    for ring in context_rings[:2]:
        ring.start(0)
    for ring in context_rings[:2]:
        ring.start(1)
    weight_ring.arrive()

    def to_twin(index, owner):
        row = pl.multiple_of(owner * share + core * half, half)
        ref = output_weight.at[pl.ds(row, half), :]
        return pltpu.make_async_remote_copy(
            src_ref=ref,
            dst_ref=ref,
            send_sem=ring_send.at[6 + index],
            recv_sem=ring_recv.at[6 + index],
            device_id={"pair": twin},
            device_id_type=MESH,
        )

    twins = [to_twin(index, owner) for index, owner in enumerate((before, after, across))]
    for copy in twins:
        copy.start()
    for ring in context_rings[:2]:
        ring.forward()
    got = spread.at[pl.ds(0, kinds // 2)]
    pltpu.make_async_copy(got, got, exchange_sem.at[3 + 1 - part]).wait()
    for ring in context_rings[2:]:
        ring.start(0)
    for ring in context_rings[2:]:
        ring.start(1)

    get_key.wait()
    get_value.wait()
    part_rows = frame_part * slots

    def project(index):
        at = part if index == 0 else 1 - part
        base = index * (normed.shape[0] // 2)
        for start in range(0, part_rows, TILE):
            count = min(TILE, part_rows - start)
            tile = context[pl.ds(at * frame_part + start // slots, count // slots)]
            normed[base + start : base + start + count, :] = normalized(
                tile.reshape(count, width).astype(F32)
            )
        for weight, target in ((key_weight, keys), (value_weight, values)):
            result = jnp.dot(
                normed[base : base + part_rows, :], weight[...], preferred_element_type=F32
            )
            for piece in range(halves):
                target[at, piece, 0:part_rows, :] = result[:, piece * LANES : (piece + 1) * LANES]

    for ring in context_rings[2:]:
        ring.forward()
    for index in range(2):
        for ring in context_rings[2 * index : 2 * index + 2]:
            ring.arrive()
        project(index)

    heads = share // HEAD_DIM

    def of_slot(source, slot):
        at = pl.ds(slot, frame_part, stride=slots)
        return jnp.concatenate([take(source.at[k], at) for k in range(2)], axis=0).astype(BF16)

    frame_keys = [of_slot(keys, slot) for slot in range(slots)]
    frame_values = [of_slot(values, slot) for slot in range(slots)]

    def attend(start, stop):
        count = -(-(stop - start) // slots // 8) * 8
        head_of = lax.broadcasted_iota(jnp.int32, (count, share), 1) // HEAD_DIM
        for slot in range(slots):
            at = pl.ds(start + slot, count, stride=slots)
            query = take(queries, at)
            stacked = jnp.concatenate(
                [jnp.where(head_of == head, query, 0.0) for head in range(heads)], axis=0
            ).astype(BF16)
            scores = (
                lax.dot_general(
                    stacked,
                    frame_keys[slot],
                    (((1,), (1,)), ((), ())),
                    preferred_element_type=F32,
                )
                * HEAD_DIM ** (-0.5)
            )
            lifted = jnp.exp(scores - jnp.max(scores, axis=-1, keepdims=True))
            weights = (lifted * (1.0 / jnp.sum(lifted, axis=-1, keepdims=True))).astype(BF16)
            spans = jnp.dot(weights, frame_values[slot], preferred_element_type=F32)
            total = spans[:count]
            for head in range(1, heads):
                total = jnp.where(head_of == head, spans[head * count : (head + 1) * count], total)
            for piece in range(mixed.shape[0]):
                mixed[piece, at, :] = total[:, piece * LANES : (piece + 1) * LANES]
        attended[start:stop, pl.ds(column, share)] = take(mixed, pl.ds(start, stop - start)).astype(
            BF16
        )

    for index, piece in enumerate(pieces):
        attend(*piece)
        if index < 2:
            launch(attended_rings[index])

    def sends(index, first, last):
        base = 33 + 6 * len(pieces) + 6 * index

        def copy(offset, source, peer):
            return pltpu.make_async_remote_copy(
                src_ref=source,
                dst_ref=landed.at[offset, first:last, :],
                send_sem=ring_send.at[base + offset],
                recv_sem=ring_recv.at[base + offset],
                device_id={"mp": peer},
                device_id_type=MESH,
            )

        return [
            copy(0, packed.at[first:last, lanes_of(across, 0)], after),
            copy(1, packed.at[first:last, lanes_of(across, 1)], before),
            copy(2, packed.at[first:last, lanes_of(after, 1)], after),
            copy(3, packed.at[first:last, lanes_of(before, 0)], before),
            copy(4, summed.at[0, first:last, :], after),
            copy(5, summed.at[1, first:last, :], before),
        ]

    reductions = [sends(index, *piece) for index, piece in enumerate(pieces)]

    def mix(index):
        first, last = pieces[index]
        hidden[first:last, :] = flat[first:last, :].astype(F32) + jnp.dot(
            attended[first:last, :], output_weight[...], preferred_element_type=F32
        )
        normalize(hidden, normed, first, last)
        expanded = gelu(
            jnp.dot(normed[first:last, :], up_weight[...], preferred_element_type=F32)
        ).astype(BF16)
        result = jnp.dot(expanded, down_weight[...], preferred_element_type=F32)
        partial[first:last, :] = result
        packed[first:last, :] = result.astype(BF16)
        for copy in reductions[index][:4]:
            copy.start()

    def relay(index):
        first, last = pieces[index]
        for piece, owner in ((0, after), (1, before)):
            reductions[index][piece].wait_recv()
            summed[piece, first:last, :] = (
                partial[first:last, lanes_of(owner, piece)]
                + landed[piece, first:last, :].astype(F32)
            ).astype(BF16)
            reductions[index][4 + piece].start()

    def finish(index):
        first, last = pieces[index]
        for copy in reductions[index][2:]:
            copy.wait_recv()
        for piece, others in ((0, (4, 3)), (1, (2, 5))):
            result = partial[first:last, lanes_of(rank, piece)]
            for other in others:
                result = result + landed[other, first:last, :].astype(F32)
            row = first + lax.broadcasted_iota(jnp.int32, result.shape, 0)
            limit = table_ref[groups * slots]
            for slot in range(1, slots):
                limit = jnp.where(lax.rem(row, slots) == slot, table_ref[groups * slots + slot], limit)
            result = hidden[first:last, lanes_of(rank, piece)] + result
            result = jnp.where(row // slots < limit, result, 0.0).astype(BF16)
            out_ref[
                first // slots : last // slots, :, piece * LANES : (piece + 1) * LANES
            ] = result.reshape((last - first) // slots, slots, LANES)

    for index in range(last_piece):
        attended_rings[index].forward()
        if index + 2 <= last_piece:
            launch(attended_rings[index + 2])
    for copy in twins:
        copy.wait_recv()
    get_up.wait()
    get_down.wait()
    for index, ring in enumerate(attended_rings):
        ring.arrive()
        mix(index)
        if index == 0:
            attended_rings[last_piece].forward()
        else:
            relay(index - 1)
    for index in range(last_piece - 1):
        finish(index)
    relay(last_piece)
    for index in range(last_piece - 1, last_piece + 1):
        finish(index)

    for ring in [weight_ring] + context_rings + attended_rings:
        ring.settle()
    for copy in twins + sum(reductions, []):
        copy.wait_send()

    @pl.when(keeps)
    def _():
        left = spread.at[pl.ds(0, kinds - 1)]
        pltpu.make_async_copy(left, left, exchange_sem.at[0]).wait()
        sent = spread.at[pl.ds(0, groups - 1)]
        pltpu.make_async_copy(sent, sent, exchange_sem.at[2]).wait()

    @pl.when(jnp.logical_not(keeps))
    def _():
        left = spread.at[pl.ds(0, kinds)]
        pltpu.make_async_copy(left, left, exchange_sem.at[0]).wait()


def body(
    current,
    past_tokens,
    counts,
    partners,
    query_weight,
    key_weight,
    value_weight,
    output_weight,
    up_weight,
    down_weight,
):
    slots, frame, width = current.shape
    groups, shards = lax.axis_size("pair"), lax.axis_size("mp")
    share = width // shards
    features = query_weight.shape[1]
    hidden_units = up_weight.shape[1]
    rows = slots * frame
    spare = rows + TILE
    half_rows = -(-rows // 2 // TILE) * TILE
    whole = pl.BlockSpec(memory_space=pltpu.HBM)
    packed_shape = (frame, slots, width)
    semaphores = 33 + 12 * (len(CUTS) + 1)
    return pl.pallas_call(
        functools.partial(decoder_kernel, groups, shards),
        out_shape=jax.ShapeDtypeStruct((frame, slots, share), BF16),
        in_specs=[pl.BlockSpec(memory_space=pltpu.SMEM)] + [whole] * 8,
        out_specs=pl.BlockSpec(memory_space=pltpu.VMEM),
        scratch_shapes=[
            pltpu.VMEM(packed_shape, BF16),
            pltpu.VMEM(packed_shape, BF16),
            pltpu.VMEM((width, features), BF16),
            pltpu.VMEM((width, features), BF16),
            pltpu.VMEM((width, features), BF16),
            pltpu.VMEM((width, width), BF16),
            pltpu.VMEM((width, hidden_units), BF16),
            pltpu.VMEM((hidden_units, width), BF16),
            pltpu.VMEM((groups, BLOCK_ROWS, slots, LANES), BF16),
            pltpu.VMEM((groups, BLOCK_ROWS, slots, LANES), BF16),
            pltpu.VMEM(packed_shape, BF16),
            pltpu.VMEM((rows, width), BF16),
            pltpu.VMEM((2 * half_rows, width), BF16),
            pltpu.VMEM((features // LANES, spare, LANES), F32),
            pltpu.VMEM((2, features // LANES, half_rows, LANES), F32),
            pltpu.VMEM((2, features // LANES, half_rows, LANES), F32),
            pltpu.VMEM((features // LANES, spare, LANES), F32),
            pltpu.VMEM((rows, width), BF16),
            pltpu.VMEM((rows, width), F32),
            pltpu.VMEM((rows, width), F32),
            pltpu.VMEM((rows, width), BF16),
            pltpu.VMEM((2, rows, LANES), BF16),
            pltpu.VMEM((6, rows, LANES), BF16),
            pltpu.SemaphoreType.DMA((8,)),
            pltpu.SemaphoreType.DMA((5,)),
            pltpu.SemaphoreType.DMA((semaphores,)),
            pltpu.SemaphoreType.DMA((semaphores,)),
        ],
        compiler_params=pltpu.CompilerParams(
            collective_id=0, has_side_effects=True, vmem_limit_bytes=VMEM_LIMIT
        ),
        name="decoder",
    )(
        jnp.concatenate([partners, counts]),
        past_tokens.transpose(1, 0, 2),
        current.transpose(1, 0, 2),
        query_weight,
        key_weight,
        value_weight,
        output_weight,
        up_weight,
        down_weight,
    ).transpose(1, 0, 2)


def solution(mesh):
    placed = (
        P("pair", None, None),
        P("pair", None, None),
        P("pair"),
        P(),
        P(None, "mp"),
        P(None, "mp"),
        P(None, "mp"),
        P("mp", None),
        P(None, "mp"),
        P("mp", None),
    )
    return jax.shard_map(
        body, mesh=mesh, in_specs=placed, out_specs=P("pair", None, "mp"), check_vma=False
    )
```
